256 devices in a mesh: rep: 32 (over z_hi, y, x), dom: 8 (over z_lo, core).
Axes of the slice: x: 4, y: 4, z: 8 (z_hi: 2, z_lo: 4; z = z_hi * 4 + z_lo), core: 2. Of those that a mesh axis runs over, the one named last changes fastest.
Arguments:
- protein_pos: float32 [3, 524288], P(None, ('rep', 'dom')), parts along dimension 1, may hold values from -4 to 4, as said below
- protein_vel: float32 [3, 524288], P(None, ('rep', 'dom')), parts along dimension 1, may hold values from -3 to 3
- inv_mass: float32 [524288], P(('rep', 'dom')), parts along dimension 0, may hold values from 0.0625 to 1
- bond_atoms: int32 [2, 327680], P(None, ('rep', 'dom')), parts along dimension 1, may hold values from 0 to 2047, as said below
- left_atoms: int32 [98304], P(('rep', 'dom')), parts along dimension 0, may hold values from 0 to 2047, as said below
- right_atoms: int32 [98304], P(('rep', 'dom')), parts along dimension 0, may hold values from 0 to 2047, as said below
- water_pos: float32 [9, 262144], P(None, ('rep', 'dom')), parts along dimension 1, may hold values from -3.2 to 3.2, as said below
- water_vel: float32 [9, 262144], P(None, ('rep', 'dom')), parts along dimension 1, may hold values from -3 to 3
Outputs:
- protein_velocity: float32 [3, 524288], P(None, ('rep', 'dom')), parts along dimension 1
- water_velocity: float32 [9, 262144], P(None, ('rep', 'dom')), parts along dimension 1
The draws below stay inside these ranges and needn't reach their ends.
There are 32 independent parts, one for each index of `rep`. The reference program is written for one: setup_inputs(seed, part) draws one part's arguments, and reference() takes and returns one part's arrays. A program takes and returns all parts, laid end to end along the dimension named above; each array names one. Nothing has to cross between parts.
Inputs may be any that keep to these rules, and one draw needn't show every extreme that they name: `bond_atoms`: indices within the domain's block of 2048 atoms; each column joins two different atoms; together with the cross bonds the bonds form a forest. `left_atoms`: distinct indices within the domain's block, none of them in right_atoms. `right_atoms`: distinct indices within the domain's block. `protein_pos`: every bond and every cross bond joins atoms 0.1 to 0.15 apart. `water_pos`: each column holds one rigid water: oxygen, then two hydrogens, 0.09572 from the oxygen and 0.15139 from each other.
All inputs are finite; a program needn't handle non-finite values.
Results may differ from the reference program's by a relative error of at most 0.0003.
Values sent between devices are 32-bit elements; how exact they have to be, the bound alone decides.
A program may use at most 64 MiB of HBM per device.

```python
import math
import jax
import jax.numpy as jnp
from jax import lax

PROT_DEV = 2048
HALO = 384
ORDER = 4
ITER = 2
BOND_DEV = 1280
PROTEIN = 16384
BONDS = 10240
CROSS = 3072
WATERS = 8192
N_DOM = 8


oxygen_hydrogen = 0.09572


hydrogen_pair = 0.15139


def topology(key):
    base = jax.random.fold_in(key, 7)
    perms = jax.vmap(lambda single: jax.random.permutation(single, PROT_DEV))(jax.random.split(base, N_DOM)).astype(jnp.int32)
    mains = BOND_DEV - HALO
    nodes = jnp.arange(mains + 1, dtype=jnp.int32)
    parents = jnp.broadcast_to(jnp.maximum(nodes - 1, 0) // 3, (N_DOM, mains + 1)).astype(jnp.int32)
    return (perms, parents)


def draw_bond_atoms(key, part):
    perms, parents = topology(key)
    mains = BOND_DEV - HALO
    nodes = jnp.arange(1, mains + 1, dtype=jnp.int32)
    child_main = perms[:, HALO + 1:HALO + 1 + mains]
    parent_main = jnp.take_along_axis(perms, parents[:, nodes] + HALO, axis=1)
    child_cap = perms[:, HALO + mains + 1:HALO + mains + 1 + HALO]
    parent_cap = perms[:, :HALO]
    child = jnp.concatenate([child_main, child_cap], axis=1)
    parent = jnp.concatenate([parent_main, parent_cap], axis=1)
    return jnp.stack([child, parent]).reshape(2, N_DOM * BOND_DEV).astype(jnp.int32)


def draw_left_atoms(key, part):
    perms, parents = topology(key)
    return perms[:, :HALO].reshape(N_DOM * HALO).astype(jnp.int32)


def draw_right_atoms(key, part):
    perms, parents = topology(key)
    mains = BOND_DEV - HALO
    return perms[:, mains + 1:mains + 1 + HALO].reshape(N_DOM * HALO).astype(jnp.int32)


def bond_lengths(key, shape):
    return jnp.exp(jax.random.uniform(key, shape, jnp.float32, math.log(0.1), math.log(0.15)))


def random_steps(key, shape):
    keys = jax.random.split(key, 3)
    cosine = jax.random.uniform(keys[0], shape, jnp.float32, -1.0, 1.0)
    angle = jax.random.uniform(keys[1], shape, jnp.float32, 0.0, 2.0 * math.pi)
    sine = jnp.sqrt(jnp.maximum(1.0 - cosine * cosine, 0.0))
    lengths = bond_lengths(keys[2], shape)
    return jnp.stack([sine * jnp.cos(angle), sine * jnp.sin(angle), cosine], axis=1) * lengths[:, None, :]


def tetra_steps(key, index, sign):
    keys = jax.random.split(key, 2)
    table = jnp.array([[1.0, 1.0, 1.0], [1.0, -1.0, -1.0], [-1.0, 1.0, -1.0], [-1.0, -1.0, 1.0]], jnp.float32) / math.sqrt(3.0)
    pick = (index[..., None] == jnp.arange(4, dtype=jnp.int32)).astype(jnp.float32)
    direction = jnp.einsum('dnk,kc->dcn', pick, table) * sign[:, None, :]
    jitter = jnp.clip(jax.random.normal(keys[0], direction.shape, jnp.float32), -2.0, 2.0)
    direction = direction + 0.15 * jitter
    direction = direction / jnp.sqrt(jnp.sum(direction * direction, axis=1, keepdims=True))
    return direction * bond_lengths(keys[1], index.shape)[:, None, :]


def draw_protein_pos(key, part):
    perms, parents = topology(key)
    keys = jax.random.split(jax.random.fold_in(key, 21), 9)
    mains = BOND_DEV - HALO
    nodes = jnp.arange(mains + 1, dtype=jnp.int32)
    turns = jax.random.randint(keys[5], (N_DOM, mains + 1), 0, 3, dtype=jnp.int32)
    first_dir = jax.random.randint(keys[6], (N_DOM, 1), 0, 4, dtype=jnp.int32)
    slot = jnp.maximum(nodes - 1, 0) % 3
    index = jnp.broadcast_to(first_dir, (N_DOM, mains + 1)).astype(jnp.int32)
    depth = jnp.zeros((N_DOM, mains + 1), jnp.int32)
    for rounds in range(16):
        up_index = jnp.take_along_axis(index, parents, axis=1)
        up_turn = jnp.take_along_axis(turns, parents, axis=1)
        up_depth = jnp.take_along_axis(depth, parents, axis=1)
        index = jnp.where(nodes == 0, first_dir, (up_index + 1 + (slot + up_turn) % 3) % 4).astype(jnp.int32)
        depth = jnp.where(nodes == 0, 0, up_depth + 1).astype(jnp.int32)
    sign = jnp.where(depth % 2 == 1, 1.0, -1.0).astype(jnp.float32)
    steps = tetra_steps(keys[0], index, sign)
    steps = steps.at[:, :, 0].set(0.0)
    root = jax.random.uniform(keys[1], (N_DOM, 3), jnp.float32, -1.0, 1.0)
    total = steps
    pointer = parents
    for rounds in range(6):
        total = total + jnp.take_along_axis(total, jnp.broadcast_to(pointer[:, None, :], total.shape), axis=2)
        pointer = jnp.take_along_axis(pointer, pointer, axis=1)
    main_pos = total + root[:, :, None]
    anchor_pos = main_pos[:, :, mains + 1 - HALO:mains + 1]
    anchor_index = jnp.roll(index[:, mains + 1 - HALO:mains + 1], 1, axis=0)
    anchor_depth = jnp.roll(depth[:, mains + 1 - HALO:mains + 1], 1, axis=0)
    anchor_sign = jnp.where(anchor_depth % 2 == 0, 1.0, -1.0).astype(jnp.float32)
    cap_index = (anchor_index + 1 + jax.random.randint(keys[7], (N_DOM, HALO), 0, 3, dtype=jnp.int32)) % 4
    child_index = (cap_index + 1 + jax.random.randint(keys[8], (N_DOM, HALO), 0, 3, dtype=jnp.int32)) % 4
    cap_pos = jnp.roll(anchor_pos, 1, axis=0) + tetra_steps(keys[2], cap_index, anchor_sign)
    child_pos = cap_pos + tetra_steps(keys[3], child_index, -anchor_sign)
    lone_pos = root[:, :, None] + random_steps(keys[4], (N_DOM, HALO - 1))

    def place(perm, main_part, cap_part, child_part, lone_part):
        field = jnp.zeros((3, PROT_DEV), jnp.float32)
        field = field.at[:, perm[HALO:HALO + mains + 1]].set(main_part)
        field = field.at[:, perm[:HALO]].set(cap_part)
        field = field.at[:, perm[HALO + mains + 1:HALO + mains + 1 + HALO]].set(child_part)
        return field.at[:, perm[PROT_DEV - HALO + 1:]].set(lone_part)
    placed = jax.vmap(place)(perms, main_pos, cap_pos, child_pos, lone_pos)
    return jnp.transpose(placed, (1, 0, 2)).reshape(3, N_DOM * PROT_DEV)


def draw_water_pos(key, part):
    keys = jax.random.split(jax.random.fold_in(key, 31), 4)
    oxygen = jax.random.uniform(keys[0], (3, WATERS), jnp.float32, -3.0, 3.0)
    first_angle = jax.random.uniform(keys[1], (WATERS,), jnp.float32, -math.pi, math.pi)
    second_angle = jax.random.uniform(keys[2], (WATERS,), jnp.float32, -math.pi, math.pi)
    third_angle = jax.random.uniform(keys[3], (WATERS,), jnp.float32, -math.pi, math.pi)
    cos_a, sin_a = (jnp.cos(first_angle), jnp.sin(first_angle))
    cos_b, sin_b = (jnp.cos(second_angle), jnp.sin(second_angle))
    cos_c, sin_c = (jnp.cos(third_angle), jnp.sin(third_angle))
    column_one = jnp.stack([cos_a * cos_c - sin_a * cos_b * sin_c, sin_a * cos_c + cos_a * cos_b * sin_c, sin_b * sin_c])
    column_two = jnp.stack([-cos_a * sin_c - sin_a * cos_b * cos_c, -sin_a * sin_c + cos_a * cos_b * cos_c, sin_b * cos_c])
    half = 0.5 * hydrogen_pair
    height = math.sqrt(oxygen_hydrogen * oxygen_hydrogen - half * half)
    first = oxygen + half * column_one - height * column_two
    second = oxygen - half * column_one - height * column_two
    return jnp.concatenate([oxygen, first, second], axis=0)


def block_levels(own_key, shape, shards, least, high):
    gain = 1.0
    for axis_at, shards_of in shards:
        draws = jax.random.uniform(jax.random.fold_in(jax.random.fold_in(own_key, 6), axis_at), (shards_of,), jnp.float32, least / len(shards), high / len(shards))
        gain = gain * jnp.repeat(jnp.exp(draws), shape[axis_at] // shards_of).reshape((-1,) + (1,) * (len(shape) - 1 - axis_at))
    return gain


def gaussian(key, dims, spread, bound, cuts=(), kind=jnp.bfloat16):
    level = block_levels(key, dims, cuts, -0.22, 0.18) if cuts else 1.0
    entries = jax.random.normal(key, dims, jnp.float32) * spread * level
    return jnp.minimum(jnp.maximum(entries, -bound), bound).astype(kind)


def setup_inputs(seed: int = 0, part: int = 0) -> dict:
    seeds = jax.random.split(jax.random.key(seed), 9)
    part_splits = jax.random.split(jax.random.fold_in(seeds[8], part), 9)
    return {
        "protein_pos": draw_protein_pos(jax.random.fold_in(jax.random.fold_in(seeds[8], part), 71), part),
        "protein_vel": gaussian(part_splits[1], (3, PROTEIN), 1.0, 3.0, ((1, 8),), jnp.float32),
        "inv_mass": jnp.clip(jnp.exp(math.log(1.0) - 2.7725887 * jax.random.uniform(part_splits[2], (PROTEIN,), jnp.float32) ** block_levels(part_splits[2], (PROTEIN,), ((0, 8),), -0.2, 0.2)), 0.0625, 1.0),
        "bond_atoms": draw_bond_atoms(jax.random.fold_in(jax.random.fold_in(seeds[8], part), 71), part),
        "left_atoms": draw_left_atoms(jax.random.fold_in(jax.random.fold_in(seeds[8], part), 71), part),
        "right_atoms": draw_right_atoms(jax.random.fold_in(jax.random.fold_in(seeds[8], part), 71), part),
        "water_pos": draw_water_pos(jax.random.fold_in(jax.random.fold_in(seeds[8], part), 71), part),
        "water_vel": gaussian(part_splits[7], (9, WATERS), 1.0, 3.0, ((1, 8),), jnp.float32),
    }


time_step = 0.002
mass_oxygen = 15.9994
mass_hydrogen = 1.008
oxygen_hydrogen = 0.09572
hydrogen_pair = 0.15139
total_mass = mass_oxygen + 2.0 * mass_hydrogen
half_pair = 0.5 * hydrogen_pair
water_height = math.sqrt(oxygen_hydrogen * oxygen_hydrogen - half_pair * half_pair)
oxygen_reach = 2.0 * mass_hydrogen * water_height / total_mass
hydrogen_reach = water_height - oxygen_reach

def cross_product(left, right):
    return jnp.stack([left[1] * right[2] - left[2] * right[1], left[2] * right[0] - left[0] * right[2], left[0] * right[1] - left[1] * right[0]])

def inner(left, right):
    return lax.optimization_barrier(jnp.sum(left * right, axis=0))

def settle(before, after):
    old_oxygen, old_first, old_second = (before[0:3], before[3:6], before[6:9])
    new_oxygen, new_first, new_second = (after[0:3], after[3:6], after[6:9])
    center = (mass_oxygen * new_oxygen + mass_hydrogen * (new_first + new_second)) / total_mass
    old_b = old_first - old_oxygen
    old_c = old_second - old_oxygen
    rel_a = new_oxygen - center
    rel_b = new_first - center
    rel_c = new_second - center
    normal = cross_product(old_b, old_c)
    side = cross_product(rel_a, normal)
    upward = cross_product(normal, side)
    axis_z = normal / jnp.sqrt(inner(normal, normal))
    axis_x = side / jnp.sqrt(inner(side, side))
    axis_y = upward / jnp.sqrt(inner(upward, upward))
    oldb_x = inner(axis_x, old_b)
    oldb_y = inner(axis_y, old_b)
    oldc_x = inner(axis_x, old_c)
    oldc_y = inner(axis_y, old_c)
    newa_z = inner(axis_z, rel_a)
    newb_x = inner(axis_x, rel_b)
    newb_y = inner(axis_y, rel_b)
    newb_z = inner(axis_z, rel_b)
    newc_x = inner(axis_x, rel_c)
    newc_y = inner(axis_y, rel_c)
    newc_z = inner(axis_z, rel_c)
    sin_phi = newa_z / oxygen_reach
    cos_phi = jnp.sqrt(1.0 - sin_phi * sin_phi)
    sin_psi = (newb_z - newc_z) / (2.0 * half_pair * cos_phi)
    cos_psi = jnp.sqrt(1.0 - sin_psi * sin_psi)
    rest_ay = oxygen_reach * cos_phi
    rest_bx = -half_pair * cos_psi
    lowered = -hydrogen_reach * cos_phi
    tilted = half_pair * sin_psi * sin_phi
    rest_by = lowered - tilted
    rest_cy = lowered + tilted
    alpha = rest_bx * (oldb_x - oldc_x) + oldb_y * rest_by + oldc_y * rest_cy
    beta = rest_bx * (oldc_y - oldb_y) + oldb_x * rest_by + oldc_x * rest_cy
    gamma = oldb_x * newb_y - newb_x * oldb_y + oldc_x * newc_y - newc_x * oldc_y
    summed = alpha * alpha + beta * beta
    sin_theta = (alpha * gamma - beta * jnp.sqrt(summed - gamma * gamma)) / summed
    cos_theta = jnp.sqrt(1.0 - sin_theta * sin_theta)
    final_ax = -rest_ay * sin_theta
    final_ay = rest_ay * cos_theta
    final_bx = rest_bx * cos_theta - rest_by * sin_theta
    final_by = rest_bx * sin_theta + rest_by * cos_theta
    final_cx = -rest_bx * cos_theta - rest_cy * sin_theta
    final_cy = -rest_bx * sin_theta + rest_cy * cos_theta
    oxygen = center + axis_x * final_ax + axis_y * final_ay + axis_z * newa_z
    first = center + axis_x * final_bx + axis_y * final_by + axis_z * newb_z
    second = center + axis_x * final_cx + axis_y * final_cy + axis_z * newc_z
    return jnp.concatenate([oxygen, first, second], axis=0)

def reference(protein_pos, protein_vel, inv_mass, bond_atoms, left_atoms, right_atoms, water_pos, water_vel):
    bond_domain = jnp.arange(BONDS, dtype=jnp.int32) // BOND_DEV
    slot_domain = jnp.arange(CROSS, dtype=jnp.int32) // HALO
    next_domain = (slot_domain + 1) % N_DOM
    anchors = right_atoms + slot_domain * PROT_DEV
    capped = jnp.roll(left_atoms, -HALO) + next_domain * PROT_DEV
    first = jnp.concatenate([bond_atoms[0] + bond_domain * PROT_DEV, anchors]).astype(jnp.int32)
    second = jnp.concatenate([bond_atoms[1] + bond_domain * PROT_DEV, capped]).astype(jnp.int32)
    moved = protein_pos + time_step * protein_vel
    diff = protein_pos[:, first] - protein_pos[:, second]
    length = jnp.sqrt(inner(diff, diff))
    unit = diff / length
    scale = 1.0 / jnp.sqrt(inv_mass[first] + inv_mass[second])

    def atom_field(values):
        weighted = unit * (scale * values)
        force = jnp.zeros((3, PROTEIN), jnp.float32).at[:, first].add(weighted).at[:, second].add(-weighted)
        return inv_mass * force

    def expand(rhs):
        total = rhs
        current = rhs
        for order_index in range(ORDER):
            field = atom_field(current)
            current = current - scale * inner(unit, field[:, first] - field[:, second])
            total = total + current
        return total
    rhs = scale * (inner(unit, moved[:, first] - moved[:, second]) - length)
    delta = -atom_field(expand(rhs))
    for round_index in range(ITER):
        now = moved + delta
        gap = now[:, first] - now[:, second]
        target = jnp.sqrt(2.0 * length * length - inner(gap, gap))
        rhs = scale * (length - target)
        delta = delta - atom_field(expand(rhs))
    protein_velocity = protein_vel + delta / time_step
    water_moved = water_pos + time_step * water_vel
    settled = settle(water_pos, water_moved)
    water_velocity = water_vel + (settled - water_moved) / time_step
    return (protein_velocity, water_velocity)
```

```python
import math

import jax
import jax.numpy as jnp
from jax import lax
from jax.experimental import pallas as pl
from jax.experimental.pallas import tpu as pltpu
from jax.sharding import PartitionSpec as P

ORDER = 4
ITER = 2

time_step = 0.002
mass_oxygen = 15.9994
mass_hydrogen = 1.008
oxygen_hydrogen = 0.09572
hydrogen_pair = 0.15139
total_mass = mass_oxygen + 2.0 * mass_hydrogen
half_pair = 0.5 * hydrogen_pair
water_height = math.sqrt(oxygen_hydrogen * oxygen_hydrogen - half_pair * half_pair)
oxygen_reach = 2.0 * mass_hydrogen * water_height / total_mass
hydrogen_reach = water_height - oxygen_reach

E = 20
S = 6
DIFF, DVEL, SCALE, MASS, PIDX, CONT, CIDX = 0, 3 * E, 6 * E, 7 * E, 8 * E, 9 * E, 10 * E
SPOS = 11 * E
SVEL, SMASS, SIDX = SPOS + 3 * S, SPOS + 6 * S, SPOS + 7 * S
ROWS = 272
f32, i32 = jnp.float32, jnp.int32


def take(table, lanes):
    return jnp.take_along_axis(table, lanes, axis=1, mode="promise_in_bounds")


def cross3(a, b):
    return (
        a[1] * b[2] - a[2] * b[1],
        a[2] * b[0] - a[0] * b[2],
        a[0] * b[1] - a[1] * b[0],
    )


def dot3(a, b):
    return a[0] * b[0] + a[1] * b[1] + a[2] * b[2]


def settle(old, vel):
    old_b = [old[3 + k] - old[k] for k in range(3)]
    old_c = [old[6 + k] - old[k] for k in range(3)]
    new_a = [time_step * vel[k] for k in range(3)]
    new_b = [old_b[k] + time_step * vel[3 + k] for k in range(3)]
    new_c = [old_c[k] + time_step * vel[6 + k] for k in range(3)]
    center = [
        (mass_oxygen * new_a[k] + mass_hydrogen * (new_b[k] + new_c[k])) / total_mass
        for k in range(3)
    ]
    rel_a = [new_a[k] - center[k] for k in range(3)]
    rel_b = [new_b[k] - center[k] for k in range(3)]
    rel_c = [new_c[k] - center[k] for k in range(3)]
    normal = cross3(old_b, old_c)
    side = cross3(rel_a, normal)
    upward = cross3(normal, side)

    def norm(vec):
        size = jnp.sqrt(dot3(vec, vec))
        return [part / size for part in vec]

    axis_z, axis_x, axis_y = norm(normal), norm(side), norm(upward)
    oldb_x, oldb_y = dot3(axis_x, old_b), dot3(axis_y, old_b)
    oldc_x, oldc_y = dot3(axis_x, old_c), dot3(axis_y, old_c)
    newa_z = dot3(axis_z, rel_a)
    newb_x, newb_y, newb_z = dot3(axis_x, rel_b), dot3(axis_y, rel_b), dot3(axis_z, rel_b)
    newc_x, newc_y, newc_z = dot3(axis_x, rel_c), dot3(axis_y, rel_c), dot3(axis_z, rel_c)
    sin_phi = newa_z / oxygen_reach
    cos_phi = jnp.sqrt(1.0 - sin_phi * sin_phi)
    sin_psi = (newb_z - newc_z) / (2.0 * half_pair * cos_phi)
    cos_psi = jnp.sqrt(1.0 - sin_psi * sin_psi)
    rest_ay = oxygen_reach * cos_phi
    rest_bx = -half_pair * cos_psi
    lowered = -hydrogen_reach * cos_phi
    tilted = half_pair * sin_psi * sin_phi
    rest_by = lowered - tilted
    rest_cy = lowered + tilted
    alpha = rest_bx * (oldb_x - oldc_x) + oldb_y * rest_by + oldc_y * rest_cy
    beta = rest_bx * (oldc_y - oldb_y) + oldb_x * rest_by + oldc_x * rest_cy
    gamma = oldb_x * newb_y - newb_x * oldb_y + oldc_x * newc_y - newc_x * oldc_y
    summed = alpha * alpha + beta * beta
    sin_theta = (alpha * gamma - beta * jnp.sqrt(summed - gamma * gamma)) / summed
    cos_theta = jnp.sqrt(1.0 - sin_theta * sin_theta)
    final_ax = -rest_ay * sin_theta
    final_ay = rest_ay * cos_theta
    final_bx = rest_bx * cos_theta - rest_by * sin_theta
    final_by = rest_bx * sin_theta + rest_by * cos_theta
    final_cx = -rest_bx * cos_theta - rest_cy * sin_theta
    final_cy = -rest_bx * sin_theta + rest_cy * cos_theta
    out = []
    for rel, along_x, along_y, along_z in (
        (rel_a, final_ax, final_ay, newa_z),
        (rel_b, final_bx, final_by, newb_z),
        (rel_c, final_cx, final_cy, newc_z),
    ):
        for k in range(3):
            out.append(axis_x[k] * along_x + axis_y[k] * along_y + axis_z[k] * along_z - rel[k])
    return [vel[k] + out[k] / time_step for k in range(9)]


def sort4(x):
    lane = lax.broadcasted_iota(i32, (8, 128), 1)
    sub = lax.broadcasted_iota(i32, (8, 128), 0)
    within = (lane << 5) | (sub << 2)
    x = list(x)
    for k in range(1, 13):
        for j in range(k - 1, -1, -1):
            if j < 2:
                for a in range(4):
                    b = a | (1 << j)
                    if a == b:
                        continue
                    low, high = jnp.minimum(x[a], x[b]), jnp.maximum(x[a], x[b])
                    if k == 12:
                        x[a], x[b] = low, high
                    elif k < 2:
                        x[a], x[b] = (low, high) if not (a >> k) & 1 else (high, low)
                    else:
                        up = ((within >> k) & 1) == 0
                        x[a], x[b] = jnp.where(up, low, high), jnp.where(up, high, low)
                continue
            first = ((within >> j) & 1) == 0
            if k == 12:
                keep_low = first
            else:
                keep_low = ((within >> j) & 1) == ((within >> k) & 1)
            for a in range(4):
                if j < 5:
                    step = 1 << (j - 2)
                    if step == 4:
                        other = pltpu.roll(x[a], 4, 0)
                    else:
                        other = jnp.where(
                            first, pltpu.roll(x[a], 8 - step, 0), pltpu.roll(x[a], step, 0)
                        )
                else:
                    other = take(x[a], lane ^ (1 << (j - 5)))
                x[a] = jnp.where(keep_low, jnp.minimum(x[a], other), jnp.maximum(x[a], other))
    return x


def gather_rows(tables, count, rows, lanes):
    outs = []
    for row_at, lane_at in zip(rows, lanes):
        hits = [row_at == r for r in range(count)]
        got = []
        for table in tables:
            acc = jnp.zeros((8, 128), table(0).dtype)
            for r in range(count):
                acc = jnp.where(hits[r], take(table(r), lane_at), acc)
            got.append(acc)
        outs.append(got)
    return outs


def row_of(ref, *base):
    def read(r):
        return jnp.broadcast_to(ref[base + (pl.ds(r, 1),)] if base else ref[pl.ds(r, 1), :], (8, 128))

    return read


def prepare(
    pos, vel, mass, bonds, left, right, wpos, wvel, block, local, wout,
    table, ends, keys, atoms, before, slots, water,
):
    lane = lax.broadcasted_iota(i32, (8, 128), 1)
    sub = lax.broadcasted_iota(i32, (8, 128), 0)
    for r in range(16):
        at = pl.ds(128 * r, 128)
        for k in range(3):
            table[k, pl.ds(r, 1)] = pos[pl.ds(k, 1), at]
            table[3 + k, pl.ds(r, 1)] = vel[pl.ds(k, 1), at]
        table[6, pl.ds(r, 1)] = mass[pl.ds(r, 1), :]
    for half in range(2):
        ends[pl.ds(16 * half + 8, 8), :] = jnp.full((8, 128), 2048, i32)
        for r in range(10):
            ends[pl.ds(16 * half + r, 1), :] = bonds[pl.ds(half, 1), pl.ds(128 * r, 128)]
    slots[...] = jnp.zeros((8, 128), i32)
    for r in range(3):
        slots[pl.ds(r, 1), :] = right[pl.ds(r, 1), :]
        slots[pl.ds(3 + r, 1), :] = left[pl.ds(r, 1), :]

    start = []
    for q in range(4):
        at = sub + 8 * q
        start.append((ends[pl.ds(8 * q, 8), :] << 12) | (at << 7) | lane)
    done = sort4(start)
    for q in range(4):
        before[pl.ds(8 * q, 8), :] = done[q]
    rows, lanes = [], []
    for q in range(3):
        n = jnp.minimum(lane * E + sub + 8 * q, 4095)
        rows.append(((n & 3) << 3) | ((n >> 2) & 7))
        lanes.append(n >> 5)
    key = [g[0] for g in gather_rows([row_of(before)], 32, rows, lanes)]
    for q in range(3):
        keys[pl.ds(8 * q, 8), :] = key[q]
    atom = [k >> 12 for k in key]
    twin = [(k & 4095) ^ 2048 for k in key]
    other = [
        g[0]
        for g in gather_rows([row_of(ends)], 26, [t >> 7 for t in twin], [t & 127 for t in twin])
    ]

    slot_atom = slots[...]
    own_atom = [(sub + 8 * q) * 128 + lane for q in range(2)]
    queries = [(other[q] << 12) | twin[q] for q in range(3)]
    queries += [(a << 12) | 4095 for a in [slot_atom] + own_atom]
    leaders = jnp.broadcast_to(keys[pl.ds(0, 1), :], (8, 128))
    found_row, found_lane, found_key = [], [], []
    for query in queries:
        low = jnp.zeros((8, 128), i32)
        for bit in (64, 32, 16, 8, 4, 2, 1):
            low = jnp.where(take(leaders, low + bit) <= query, low + bit, low)
        count = jnp.full((8, 128), -1, i32)
        best = jnp.full((8, 128), -1, i32)
        for r in range(E):
            seen = take(jnp.broadcast_to(keys[pl.ds(r, 1), :], (8, 128)), low)
            less = seen <= query
            count = jnp.where(less, count + 1, count)
            best = jnp.where(less, seen, best)
        found_row.append(count)
        found_lane.append(low)
        found_key.append(best)
    places = [found_row[q] * 128 + found_lane[q] for q in range(6)]
    slot_place = jnp.where((found_key[3] >> 12) == slot_atom, places[3], -1)
    for q in range(2):
        place = jnp.where((found_key[4 + q] >> 12) == own_atom[q], places[4 + q], -1)
        local[pl.ds(8 * q, 8), :] = place.astype(f32)

    high = lax.broadcasted_iota(i32, (16, 128), 0)
    code = lax.broadcasted_iota(i32, (16, 128), 1) + 1
    low_of = lax.broadcasted_iota(i32, (128, 128), 0)
    which = jnp.zeros((32, 128), f32)
    for r in range(S):
        here = slots[pl.ds(r, 1), :]
        mine = jnp.broadcast_to(here >> 7, (16, 128)) == high
        left_side = jnp.concatenate(
            [jnp.where(mine, code, 0).astype(f32), jnp.where(mine, r + 1, 0).astype(f32)], axis=0
        )
        right_side = jnp.where(jnp.broadcast_to(here & 127, (128, 128)) == low_of, 1.0, 0.0)
        which = which + lax.dot_general(
            left_side.astype(jnp.bfloat16),
            right_side.astype(jnp.bfloat16),
            (((1,), (1,)), ((), ())),
            preferred_element_type=f32,
        )
    local[pl.ds(16, 16), :] = jnp.where(
        which[0:16] > 0.0, which[16:32] * 128.0 + which[0:16] - 129.0, -1.0
    )

    for q in range(3):
        atoms[pl.ds(8 * q, 8), :] = atom[q]
    before[pl.ds(0, 1), :] = pltpu.roll(atoms[pl.ds(E - 1, 1), :], 1, 1)
    before[pl.ds(1, E - 1), :] = atoms[pl.ds(0, E - 1), :]
    own_rows, own_lanes = [a >> 7 for a in atom], [a & 127 for a in atom]
    tables = [row_of(table, k) for k in range(7)] + [row_of(local.at[pl.ds(16, 16)])]
    own = gather_rows(tables, 16, own_rows, own_lanes)
    far = gather_rows(tables[:7], 16, [a >> 7 for a in other], [a & 127 for a in other])
    for q in range(3):
        size = min(8, E - 8 * q)

        def put(base, value):
            block[pl.ds(base + 8 * q, size), :] = value[0:size]

        for k in range(3):
            put(DIFF + E * k, own[q][k] - far[q][k])
            put(DVEL + E * k, own[q][3 + k] - far[q][3 + k])
        put(SCALE, 1.0 / jnp.sqrt(own[q][6] + far[q][6]))
        put(MASS, own[q][6])
        put(PIDX, places[q].astype(f32))
        same = before[pl.ds(8 * q, 8), :] == atom[q]
        if q == 0:
            same = same & ((lane > 0) | (sub > 0))
        put(CONT, jnp.where(same, 1.0, 0.0))
        put(CIDX, own[q][7])
    at_slots = gather_rows(tables[:7], 16, [slot_atom >> 7], [slot_atom & 127])[0]
    for k in range(7):
        block[pl.ds(SPOS + S * k, S), :] = at_slots[k][0:S]
    block[pl.ds(SIDX, S), :] = slot_place.astype(f32)[0:S]
    block[pl.ds(SIDX + S, ROWS - SIDX - S), :] = jnp.zeros((ROWS - SIDX - S, 128), f32)

    for k in range(9):
        for r in range(8):
            water[k, pl.ds(r, 1)] = wpos[pl.ds(k, 1), pl.ds(128 * r, 128)]
            water[9 + k, pl.ds(r, 1)] = wvel[pl.ds(k, 1), pl.ds(128 * r, 128)]
    new = settle([water[k] for k in range(9)], [water[9 + k] for k in range(9)])
    for k in range(9):
        water[k] = new[k]
        for r in range(8):
            wout[pl.ds(k, 1), pl.ds(128 * r, 128)] = water[k, pl.ds(r, 1)]


def pick(tables, rows, lanes):
    outs = [[] for _ in tables]
    for row_at, lane_at in zip(rows, lanes):
        hits = [row_at == r for r in range(len(tables[0]))]
        for out, table in zip(outs, tables):
            acc = jnp.zeros((8, 128), f32)
            for hit, part in zip(hits, table):
                acc = jnp.where(hit, take(part, lane_at), acc)
            out.append(acc)
    return outs


def swap(slots):
    back = [pltpu.roll(part, 7, 0) for part in slots[3:6]]
    ahead = [pltpu.roll(part, 1, 0) for part in slots[0:3]]
    return back + ahead


def rounds(
    data, local, vel, out,
    w, g, m, prow, plane, crow, clane, cont, pf, pb, x, xt, wc, d, length, scale, delta,
    sw, sm, srow, slane, sww, sx, sxt, sd, slength, sscale, sdelta,
):
    def rows_at(base, count):
        return [data[:, base + r, :] for r in range(count)]

    for base, row_ref, lane_ref, count in ((PIDX, prow, plane, E), (CIDX, crow, clane, E), (SIDX, srow, slane, S)):
        for r in range(count):
            value = data[:, base + r, :].astype(i32)
            row_ref[r] = value >> 7
            lane_ref[r] = value & 127
    keep = rows_at(CONT, E)
    run = jnp.ones((8, 128), f32)
    for r in range(E):
        cont[r] = keep[r]
        if r > 0:
            run = run * keep[r]
        pf[r] = run
    whole = run
    run = jnp.ones((8, 128), f32)
    for r in range(E - 1, -1, -1):
        pb[r] = run
        run = run * keep[r]
    extra = jnp.max(jnp.sum(whole, axis=1, keepdims=True)).astype(i32)
    opens = keep[0]
    closes = pltpu.roll(opens, 127, 1)

    def geometry(diff, dvel, s):
        far = jnp.sqrt(dot3(diff, diff))
        ratio = s / far
        weight = [ratio * part for part in diff]
        moved = [diff[k] + time_step * dvel[k] for k in range(3)]
        return far, weight, moved, time_step * dot3(weight, dvel)

    own = [rows_at(SPOS + S * k, S) for k in range(7)]
    twin = [swap(part) for part in own]
    for r in range(S):
        diff = [own[k][r] - twin[k][r] for k in range(3)]
        dvel = [own[3 + k][r] - twin[3 + k][r] for k in range(3)]
        s = 1.0 / jnp.sqrt(own[6][r] + twin[6][r])
        far, weight, moved, first = geometry(diff, dvel, s)
        for k in range(3):
            sw[k, r] = weight[k]
            sd[k, r] = moved[k]
            sdelta[k, r] = jnp.zeros((8, 128), f32)
        sm[r] = own[6][r]
        sww[r] = dot3(weight, weight)
        slength[r] = far
        sscale[r] = s
        sx[r] = first
    near = pick(
        [[sw[k, r] for r in range(S)] for k in range(3)],
        [crow[r] for r in range(E)],
        [clane[r] for r in range(E)],
    )
    for r in range(E):
        diff = [data[:, DIFF + E * k + r, :] for k in range(3)]
        dvel = [data[:, DVEL + E * k + r, :] for k in range(3)]
        s = data[:, SCALE + r, :]
        far, weight, moved, first = geometry(diff, dvel, s)
        for k in range(3):
            w[k, r] = weight[k]
            d[k, r] = moved[k]
            wc[k, r] = near[k][r]
            delta[k, r] = jnp.zeros((8, 128), f32)
        g[r] = dot3(weight, [near[k][r] for k in range(3)])
        m[r] = data[:, MASS + r, :]
        length[r] = far
        scale[r] = s
        x[r] = first

    def totals(parts):
        count = len(parts)
        inside = []
        for part in parts:
            acc = part[0]
            fwd = [acc]
            for r in range(1, E):
                acc = part[r] + cont[r] * acc
                fwd.append(acc)
            for r in range(E - 2, -1, -1):
                fwd[r] = jnp.where(cont[r + 1] > 0.0, fwd[r + 1], fwd[r])
            inside.append(fwd)
        ahead = tuple(opens * pltpu.roll(part[E - 1], 1, 1) for part in inside)
        back = tuple(closes * pltpu.roll(part[0], 127, 1) for part in inside)

        def spread(_, now):
            ahead_now, back_now = now[:count], now[count:]
            new = [ahead[k] + opens * pltpu.roll(whole * ahead_now[k], 1, 1) for k in range(count)]
            new += [back[k] + closes * pltpu.roll(whole * back_now[k], 127, 1) for k in range(count)]
            return tuple(new)

        carried = lax.fori_loop(0, extra, spread, ahead + back)
        return [
            [
                inside[k][r] + pf[r] * carried[k] + pb[r] * carried[count + k]
                for r in range(E)
            ]
            for k in range(count)
        ]

    def apply_k(_, carry):
        sums = totals(
            [[w[k, r] * x[r] for r in range(E)] for k in range(3)]
            + [[g[r] * x[r] for r in range(E)]]
        )
        slot_x = [sx[r] for r in range(S)]
        cross_x = pick([slot_x], [crow[r] for r in range(E)], [clane[r] for r in range(E)])[0]
        slot_sum = pick([sums[3]], [srow[r] for r in range(S)], [slane[r] for r in range(S)])[0]
        z = [
            m[r] * (w[0, r] * sums[0][r] + w[1, r] * sums[1][r] + w[2, r] * sums[2][r] + g[r] * cross_x[r])
            for r in range(E)
        ]
        slot_z = [sm[r] * (slot_sum[r] + sww[r] * slot_x[r]) for r in range(S)]
        slot_twin = swap(slot_z)
        for r in range(S):
            new = slot_x[r] - (slot_z[r] + slot_twin[r])
            sx[r] = new
            sxt[r] = sxt[r] + new
        z_twin = pick([z], [prow[r] for r in range(E)], [plane[r] for r in range(E)])[0]
        for r in range(E):
            new = x[r] - (z[r] + z_twin[r])
            x[r] = new
            xt[r] = xt[r] + new
        return carry

    def solve(index, carry):
        for r in range(E):
            xt[r] = x[r]
        for r in range(S):
            sxt[r] = sx[r]
        lax.fori_loop(0, ORDER, apply_k, 0)
        sums = totals([[w[k, r] * xt[r] for r in range(E)] for k in range(3)])
        slot_xt = [sxt[r] for r in range(S)]
        cross_x = pick([slot_xt], [crow[r] for r in range(E)], [clane[r] for r in range(E)])[0]
        slot_sum = pick(sums, [srow[r] for r in range(S)], [slane[r] for r in range(S)])
        for k in range(3):
            for r in range(E):
                delta[k, r] = delta[k, r] - m[r] * (sums[k][r] + wc[k, r] * cross_x[r])
            for r in range(S):
                sdelta[k, r] = sdelta[k, r] - sm[r] * (slot_sum[k][r] + sw[k, r] * slot_xt[r])

        @pl.when(index < ITER)
        def _():
            def lengthening(gap, far, s):
                target = jnp.sqrt(2.0 * far * far - dot3(gap, gap))
                return s * (far - target)

            here = [[delta[k, r] for r in range(E)] for k in range(3)]
            there = pick(here, [prow[r] for r in range(E)], [plane[r] for r in range(E)])
            for r in range(E):
                gap = [d[k, r] + (here[k][r] - there[k][r]) for k in range(3)]
                x[r] = lengthening(gap, length[r], scale[r])
            here = [[sdelta[k, r] for r in range(S)] for k in range(3)]
            there = [swap(part) for part in here]
            for r in range(S):
                gap = [sd[k, r] + (here[k][r] - there[k][r]) for k in range(3)]
                sx[r] = lengthening(gap, slength[r], sscale[r])

        return carry

    lax.fori_loop(0, ITER + 1, solve, 0)

    me = lax.axis_index("dom")

    def own_row(ref, k):
        return lambda r: jnp.broadcast_to(ref[k, r, pl.ds(me, 1), :], (8, 128))

    places = [local[pl.ds(8 * q, 8), :].astype(i32) for q in range(4)]
    rows, lanes = [p >> 7 for p in places], [p & 127 for p in places]
    inner = gather_rows([own_row(delta, k) for k in range(3)], E, rows[:2], lanes[:2])
    outer = gather_rows([own_row(sdelta, k) for k in range(3)], S, rows[2:], lanes[2:])
    for q in range(2):
        for k in range(3):
            xt[3 * q + k] = jnp.where(rows[q] >= 0, inner[q][k], outer[q][k])
    for k in range(3):
        for r in range(16):
            at = pl.ds(128 * r, 128)
            change = xt[3 * (r // 8) + k, pl.ds(r % 8, 1), :]
            out[pl.ds(k, 1), at] = vel[pl.ds(k, 1), at] + change / time_step


def on_device(
    protein_pos, protein_vel, inv_mass, bond_atoms, left_atoms, right_atoms, water_pos, water_vel
):
    vmem = pl.BlockSpec(memory_space=pltpu.VMEM)
    block, local, water_velocity = pl.pallas_call(
        prepare,
        out_shape=(
            jax.ShapeDtypeStruct((ROWS, 128), f32),
            jax.ShapeDtypeStruct((32, 128), f32),
            jax.ShapeDtypeStruct(water_pos.shape, f32),
        ),
        in_specs=[vmem] * 8,
        out_specs=(vmem,) * 3,
        scratch_shapes=[
            pltpu.VMEM((7, 16, 128), f32),
            pltpu.VMEM((32, 128), i32),
            pltpu.VMEM((24, 128), i32),
            pltpu.VMEM((24, 128), i32),
            pltpu.VMEM((32, 128), i32),
            pltpu.VMEM((8, 128), i32),
            pltpu.VMEM((18, 8, 128), f32),
        ],
        name="prepare",
    )(
        protein_pos,
        protein_vel,
        inv_mass.reshape(16, 128),
        bond_atoms,
        left_atoms.reshape(3, 128),
        right_atoms.reshape(3, 128),
        water_pos,
        water_vel,
    )
    data = lax.all_gather(block, "dom")
    real = [(3, E), (E,), (E,)]
    scratch = [
        ((3, E), f32), ((E,), f32), ((E,), f32),
        ((E,), i32), ((E,), i32), ((E,), i32), ((E,), i32),
        ((E,), f32), ((E,), f32), ((E,), f32),
        ((E,), f32), ((E,), f32),
        ((3, E), f32), ((3, E), f32), ((E,), f32), ((E,), f32), ((3, E), f32),
        ((3, S), f32), ((S,), f32), ((S,), i32), ((S,), i32), ((S,), f32),
        ((S,), f32), ((S,), f32), ((3, S), f32), ((S,), f32), ((S,), f32), ((3, S), f32),
    ]
    protein_velocity = pl.pallas_call(
        rounds,
        out_shape=jax.ShapeDtypeStruct(protein_vel.shape, f32),
        in_specs=[vmem] * 3,
        out_specs=vmem,
        scratch_shapes=[pltpu.VMEM(shape + (8, 128), kind) for shape, kind in scratch],
        name="rounds",
    )(data, local, protein_vel)
    return (protein_velocity, water_velocity)


def solution(mesh):
    in_specs = (
        P(None, ("rep", "dom")),
        P(None, ("rep", "dom")),
        P(("rep", "dom")),
        P(None, ("rep", "dom")),
        P(("rep", "dom")),
        P(("rep", "dom")),
        P(None, ("rep", "dom")),
        P(None, ("rep", "dom")),
    )
    out_specs = (P(None, ("rep", "dom")), P(None, ("rep", "dom")))
    return jax.shard_map(
        on_device, mesh=mesh, in_specs=in_specs, out_specs=out_specs, check_vma=False
    )
```

```python
import math

import jax
import jax.numpy as jnp
from jax import lax
from jax.experimental import pallas as pl
from jax.experimental.pallas import tpu as pltpu
from jax.sharding import PartitionSpec as P

ORDER = 4
ITER = 2

time_step = 0.002
mass_oxygen = 15.9994
mass_hydrogen = 1.008
oxygen_hydrogen = 0.09572
hydrogen_pair = 0.15139
total_mass = mass_oxygen + 2.0 * mass_hydrogen
half_pair = 0.5 * hydrogen_pair
water_height = math.sqrt(oxygen_hydrogen * oxygen_hydrogen - half_pair * half_pair)
oxygen_reach = 2.0 * mass_hydrogen * water_height / total_mass
hydrogen_reach = water_height - oxygen_reach

E = 20
S = 6
DIFF, DVEL, SCALE, MASS, PIDX, CONT, CIDX = 0, 3 * E, 6 * E, 7 * E, 8 * E, 9 * E, 10 * E
SPOS = 11 * E
SVEL, SMASS, SIDX = SPOS + 3 * S, SPOS + 6 * S, SPOS + 7 * S
ROWS = 272
f32, i32 = jnp.float32, jnp.int32


def take(table, lanes):
    return jnp.take_along_axis(table, lanes, axis=1, mode="promise_in_bounds")


def cross3(a, b):
    return (
        a[1] * b[2] - a[2] * b[1],
        a[2] * b[0] - a[0] * b[2],
        a[0] * b[1] - a[1] * b[0],
    )


def dot3(a, b):
    return a[0] * b[0] + a[1] * b[1] + a[2] * b[2]


def settle(old, vel):
    old_b = [old[3 + k] - old[k] for k in range(3)]
    old_c = [old[6 + k] - old[k] for k in range(3)]
    new_a = [time_step * vel[k] for k in range(3)]
    new_b = [old_b[k] + time_step * vel[3 + k] for k in range(3)]
    new_c = [old_c[k] + time_step * vel[6 + k] for k in range(3)]
    center = [
        (mass_oxygen * new_a[k] + mass_hydrogen * (new_b[k] + new_c[k])) / total_mass
        for k in range(3)
    ]
    rel_a = [new_a[k] - center[k] for k in range(3)]
    rel_b = [new_b[k] - center[k] for k in range(3)]
    rel_c = [new_c[k] - center[k] for k in range(3)]
    normal = cross3(old_b, old_c)
    side = cross3(rel_a, normal)
    upward = cross3(normal, side)

    def norm(vec):
        size = jnp.sqrt(dot3(vec, vec))
        return [part / size for part in vec]

    axis_z, axis_x, axis_y = norm(normal), norm(side), norm(upward)
    oldb_x, oldb_y = dot3(axis_x, old_b), dot3(axis_y, old_b)
    oldc_x, oldc_y = dot3(axis_x, old_c), dot3(axis_y, old_c)
    newa_z = dot3(axis_z, rel_a)
    newb_x, newb_y, newb_z = dot3(axis_x, rel_b), dot3(axis_y, rel_b), dot3(axis_z, rel_b)
    newc_x, newc_y, newc_z = dot3(axis_x, rel_c), dot3(axis_y, rel_c), dot3(axis_z, rel_c)
    sin_phi = newa_z / oxygen_reach
    cos_phi = jnp.sqrt(1.0 - sin_phi * sin_phi)
    sin_psi = (newb_z - newc_z) / (2.0 * half_pair * cos_phi)
    cos_psi = jnp.sqrt(1.0 - sin_psi * sin_psi)
    rest_ay = oxygen_reach * cos_phi
    rest_bx = -half_pair * cos_psi
    lowered = -hydrogen_reach * cos_phi
    tilted = half_pair * sin_psi * sin_phi
    rest_by = lowered - tilted
    rest_cy = lowered + tilted
    alpha = rest_bx * (oldb_x - oldc_x) + oldb_y * rest_by + oldc_y * rest_cy
    beta = rest_bx * (oldc_y - oldb_y) + oldb_x * rest_by + oldc_x * rest_cy
    gamma = oldb_x * newb_y - newb_x * oldb_y + oldc_x * newc_y - newc_x * oldc_y
    summed = alpha * alpha + beta * beta
    sin_theta = (alpha * gamma - beta * jnp.sqrt(summed - gamma * gamma)) / summed
    cos_theta = jnp.sqrt(1.0 - sin_theta * sin_theta)
    final_ax = -rest_ay * sin_theta
    final_ay = rest_ay * cos_theta
    final_bx = rest_bx * cos_theta - rest_by * sin_theta
    final_by = rest_bx * sin_theta + rest_by * cos_theta
    final_cx = -rest_bx * cos_theta - rest_cy * sin_theta
    final_cy = -rest_bx * sin_theta + rest_cy * cos_theta
    out = []
    for rel, along_x, along_y, along_z in (
        (rel_a, final_ax, final_ay, newa_z),
        (rel_b, final_bx, final_by, newb_z),
        (rel_c, final_cx, final_cy, newc_z),
    ):
        for k in range(3):
            out.append(axis_x[k] * along_x + axis_y[k] * along_y + axis_z[k] * along_z - rel[k])
    return [vel[k] + out[k] / time_step for k in range(9)]


def sort4(x):
    lane = lax.broadcasted_iota(i32, (8, 128), 1)
    sub = lax.broadcasted_iota(i32, (8, 128), 0)
    within = (lane << 5) | (sub << 2)
    x = list(x)
    for k in range(1, 13):
        for j in range(k - 1, -1, -1):
            if j < 2:
                for a in range(4):
                    b = a | (1 << j)
                    if a == b:
                        continue
                    low, high = jnp.minimum(x[a], x[b]), jnp.maximum(x[a], x[b])
                    if k == 12:
                        x[a], x[b] = low, high
                    elif k < 2:
                        x[a], x[b] = (low, high) if not (a >> k) & 1 else (high, low)
                    else:
                        up = ((within >> k) & 1) == 0
                        x[a], x[b] = jnp.where(up, low, high), jnp.where(up, high, low)
                continue
            first = ((within >> j) & 1) == 0
            if k == 12:
                keep_low = first
            else:
                keep_low = ((within >> j) & 1) == ((within >> k) & 1)
            for a in range(4):
                if j < 5:
                    step = 1 << (j - 2)
                    if step == 4:
                        other = pltpu.roll(x[a], 4, 0)
                    else:
                        other = jnp.where(
                            first, pltpu.roll(x[a], 8 - step, 0), pltpu.roll(x[a], step, 0)
                        )
                else:
                    other = take(x[a], lane ^ (1 << (j - 5)))
                x[a] = jnp.where(keep_low, jnp.minimum(x[a], other), jnp.maximum(x[a], other))
    return x


def gather_rows(tables, count, rows, lanes):
    outs = []
    for row_at, lane_at in zip(rows, lanes):
        hits = [row_at == r for r in range(count)]
        got = []
        for table in tables:
            acc = jnp.zeros((8, 128), table(0).dtype)
            for r in range(count):
                acc = jnp.where(hits[r], take(table(r), lane_at), acc)
            got.append(acc)
        outs.append(got)
    return outs


def row_of(ref, *base):
    def read(r):
        return jnp.broadcast_to(ref[base + (pl.ds(r, 1),)] if base else ref[pl.ds(r, 1), :], (8, 128))

    return read


def prepare(
    pos, vel, mass, bonds, left, right, wpos, wvel, block, local, wout,
    table, ends, keys, atoms, before, slots, water,
):
    lane = lax.broadcasted_iota(i32, (8, 128), 1)
    sub = lax.broadcasted_iota(i32, (8, 128), 0)
    for r in range(16):
        at = pl.ds(128 * r, 128)
        for k in range(3):
            table[k, pl.ds(r, 1)] = pos[pl.ds(k, 1), at]
            table[3 + k, pl.ds(r, 1)] = vel[pl.ds(k, 1), at]
        table[6, pl.ds(r, 1)] = mass[pl.ds(r, 1), :]
    for half in range(2):
        ends[pl.ds(16 * half + 8, 8), :] = jnp.full((8, 128), 2048, i32)
        for r in range(10):
            ends[pl.ds(16 * half + r, 1), :] = bonds[pl.ds(half, 1), pl.ds(128 * r, 128)]
    slots[...] = jnp.zeros((8, 128), i32)
    for r in range(3):
        slots[pl.ds(r, 1), :] = right[pl.ds(r, 1), :]
        slots[pl.ds(3 + r, 1), :] = left[pl.ds(r, 1), :]

    start = []
    for q in range(4):
        at = sub + 8 * q
        start.append((ends[pl.ds(8 * q, 8), :] << 12) | (at << 7) | lane)
    done = sort4(start)
    for q in range(4):
        before[pl.ds(8 * q, 8), :] = done[q]
    rows, lanes = [], []
    for q in range(3):
        n = jnp.minimum(lane * E + sub + 8 * q, 4095)
        rows.append(((n & 3) << 3) | ((n >> 2) & 7))
        lanes.append(n >> 5)
    key = [g[0] for g in gather_rows([row_of(before)], 32, rows, lanes)]
    for q in range(3):
        keys[pl.ds(8 * q, 8), :] = key[q]
    atom = [k >> 12 for k in key]
    twin = [(k & 4095) ^ 2048 for k in key]
    other = [
        g[0]
        for g in gather_rows([row_of(ends)], 26, [t >> 7 for t in twin], [t & 127 for t in twin])
    ]

    slot_atom = slots[...]
    own_atom = [(sub + 8 * q) * 128 + lane for q in range(2)]
    queries = [(other[q] << 12) | twin[q] for q in range(3)]
    queries += [(a << 12) | 4095 for a in [slot_atom] + own_atom]
    leaders = jnp.broadcast_to(keys[pl.ds(0, 1), :], (8, 128))
    found_row, found_lane, found_key = [], [], []
    for query in queries:
        low = jnp.zeros((8, 128), i32)
        for bit in (64, 32, 16, 8, 4, 2, 1):
            low = jnp.where(take(leaders, low + bit) <= query, low + bit, low)
        count = jnp.full((8, 128), -1, i32)
        best = jnp.full((8, 128), -1, i32)
        for r in range(E):
            seen = take(jnp.broadcast_to(keys[pl.ds(r, 1), :], (8, 128)), low)
            less = seen <= query
            count = jnp.where(less, count + 1, count)
            best = jnp.where(less, seen, best)
        found_row.append(count)
        found_lane.append(low)
        found_key.append(best)
    places = [found_row[q] * 128 + found_lane[q] for q in range(6)]
    slot_place = jnp.where((found_key[3] >> 12) == slot_atom, places[3], -1)
    for q in range(2):
        place = jnp.where((found_key[4 + q] >> 12) == own_atom[q], places[4 + q], -1)
        local[pl.ds(8 * q, 8), :] = place.astype(f32)

    high = lax.broadcasted_iota(i32, (16, 128), 0)
    code = lax.broadcasted_iota(i32, (16, 128), 1) + 1
    low_of = lax.broadcasted_iota(i32, (128, 128), 0)
    which = jnp.zeros((32, 128), f32)
    for r in range(S):
        here = slots[pl.ds(r, 1), :]
        mine = jnp.broadcast_to(here >> 7, (16, 128)) == high
        left_side = jnp.concatenate(
            [jnp.where(mine, code, 0).astype(f32), jnp.where(mine, r + 1, 0).astype(f32)], axis=0
        )
        right_side = jnp.where(jnp.broadcast_to(here & 127, (128, 128)) == low_of, 1.0, 0.0)
        which = which + lax.dot_general(
            left_side.astype(jnp.bfloat16),
            right_side.astype(jnp.bfloat16),
            (((1,), (1,)), ((), ())),
            preferred_element_type=f32,
        )
    local[pl.ds(16, 16), :] = jnp.where(
        which[0:16] > 0.0, which[16:32] * 128.0 + which[0:16] - 129.0, -1.0
    )

    for q in range(3):
        atoms[pl.ds(8 * q, 8), :] = atom[q]
    before[pl.ds(0, 1), :] = pltpu.roll(atoms[pl.ds(E - 1, 1), :], 1, 1)
    before[pl.ds(1, E - 1), :] = atoms[pl.ds(0, E - 1), :]
    own_rows, own_lanes = [a >> 7 for a in atom], [a & 127 for a in atom]
    tables = [row_of(table, k) for k in range(7)] + [row_of(local.at[pl.ds(16, 16)])]
    own = gather_rows(tables, 16, own_rows, own_lanes)
    far = gather_rows(tables[:7], 16, [a >> 7 for a in other], [a & 127 for a in other])
    for q in range(3):
        size = min(8, E - 8 * q)

        def put(base, value):
            block[pl.ds(base + 8 * q, size), :] = value[0:size]

        for k in range(3):
            put(DIFF + E * k, own[q][k] - far[q][k])
            put(DVEL + E * k, own[q][3 + k] - far[q][3 + k])
        put(SCALE, 1.0 / jnp.sqrt(own[q][6] + far[q][6]))
        put(MASS, own[q][6])
        put(PIDX, places[q].astype(f32))
        same = before[pl.ds(8 * q, 8), :] == atom[q]
        if q == 0:
            same = same & ((lane > 0) | (sub > 0))
        put(CONT, jnp.where(same, 1.0, 0.0))
        put(CIDX, own[q][7])
    at_slots = gather_rows(tables[:7], 16, [slot_atom >> 7], [slot_atom & 127])[0]
    for k in range(7):
        block[pl.ds(SPOS + S * k, S), :] = at_slots[k][0:S]
    block[pl.ds(SIDX, S), :] = slot_place.astype(f32)[0:S]
    block[pl.ds(SIDX + S, ROWS - SIDX - S), :] = jnp.zeros((ROWS - SIDX - S, 128), f32)

    for k in range(9):
        for r in range(8):
            water[k, pl.ds(r, 1)] = wpos[pl.ds(k, 1), pl.ds(128 * r, 128)]
            water[9 + k, pl.ds(r, 1)] = wvel[pl.ds(k, 1), pl.ds(128 * r, 128)]
    new = settle([water[k] for k in range(9)], [water[9 + k] for k in range(9)])
    for k in range(9):
        water[k] = new[k]
        for r in range(8):
            wout[pl.ds(k, 1), pl.ds(128 * r, 128)] = water[k, pl.ds(r, 1)]


def pick(tables, rows, lanes):
    outs = [[] for _ in tables]
    for row_at, lane_at in zip(rows, lanes):
        hits = [row_at == r for r in range(len(tables[0]))]
        for out, table in zip(outs, tables):
            acc = jnp.zeros((8, 128), f32)
            for hit, part in zip(hits, table):
                acc = jnp.where(hit, take(part, lane_at), acc)
            out.append(acc)
    return outs


def swap(slots):
    back = [pltpu.roll(part, 7, 0) for part in slots[3:6]]
    ahead = [pltpu.roll(part, 1, 0) for part in slots[0:3]]
    return back + ahead


def rounds(
    data, local, vel, out,
    w, g, m, prow, plane, crow, clane, cont, pf, pb, x, xt, wc, d, length, scale, delta,
    sw, sm, srow, slane, sww, sx, sxt, sd, slength, sscale, sdelta,
):
    def rows_at(base, count):
        return [data[:, base + r, :] for r in range(count)]

    for base, row_ref, lane_ref, count in ((PIDX, prow, plane, E), (CIDX, crow, clane, E), (SIDX, srow, slane, S)):
        for r in range(count):
            value = data[:, base + r, :].astype(i32)
            row_ref[r] = value >> 7
            lane_ref[r] = value & 127
    keep = rows_at(CONT, E)
    run = jnp.ones((8, 128), f32)
    for r in range(E):
        cont[r] = keep[r]
        if r > 0:
            run = run * keep[r]
        pf[r] = run
    whole = run
    run = jnp.ones((8, 128), f32)
    for r in range(E - 1, -1, -1):
        pb[r] = run
        run = run * keep[r]
    extra = jnp.max(jnp.sum(whole, axis=1, keepdims=True)).astype(i32)
    opens = keep[0]
    closes = pltpu.roll(opens, 127, 1)

    def geometry(diff, dvel, s):
        far = jnp.sqrt(dot3(diff, diff))
        ratio = s / far
        weight = [ratio * part for part in diff]
        moved = [diff[k] + time_step * dvel[k] for k in range(3)]
        return far, weight, moved, time_step * dot3(weight, dvel)

    own = [rows_at(SPOS + S * k, S) for k in range(7)]
    twin = [swap(part) for part in own]
    for r in range(S):
        diff = [own[k][r] - twin[k][r] for k in range(3)]
        dvel = [own[3 + k][r] - twin[3 + k][r] for k in range(3)]
        s = 1.0 / jnp.sqrt(own[6][r] + twin[6][r])
        far, weight, moved, first = geometry(diff, dvel, s)
        for k in range(3):
            sw[k, r] = weight[k]
            sd[k, r] = moved[k]
            sdelta[k, r] = jnp.zeros((8, 128), f32)
        sm[r] = own[6][r]
        sww[r] = dot3(weight, weight)
        slength[r] = far
        sscale[r] = s
        sx[r] = first
    near = pick(
        [[sw[k, r] for r in range(S)] for k in range(3)],
        [crow[r] for r in range(E)],
        [clane[r] for r in range(E)],
    )
    for r in range(E):
        diff = [data[:, DIFF + E * k + r, :] for k in range(3)]
        dvel = [data[:, DVEL + E * k + r, :] for k in range(3)]
        s = data[:, SCALE + r, :]
        far, weight, moved, first = geometry(diff, dvel, s)
        for k in range(3):
            w[k, r] = weight[k]
            d[k, r] = moved[k]
            wc[k, r] = near[k][r]
            delta[k, r] = jnp.zeros((8, 128), f32)
        g[r] = dot3(weight, [near[k][r] for k in range(3)])
        m[r] = data[:, MASS + r, :]
        length[r] = far
        scale[r] = s
        x[r] = first

    def totals(parts):
        count = len(parts)
        inside = []
        for part in parts:
            acc = part[0]
            fwd = [acc]
            for r in range(1, E):
                acc = part[r] + cont[r] * acc
                fwd.append(acc)
            for r in range(E - 2, -1, -1):
                fwd[r] = jnp.where(cont[r + 1] > 0.0, fwd[r + 1], fwd[r])
            inside.append(fwd)
        ahead = tuple(opens * pltpu.roll(part[E - 1], 1, 1) for part in inside)
        back = tuple(closes * pltpu.roll(part[0], 127, 1) for part in inside)

        def spread(_, now):
            ahead_now, back_now = now[:count], now[count:]
            new = [ahead[k] + opens * pltpu.roll(whole * ahead_now[k], 1, 1) for k in range(count)]
            new += [back[k] + closes * pltpu.roll(whole * back_now[k], 127, 1) for k in range(count)]
            return tuple(new)

        carried = lax.fori_loop(0, extra, spread, ahead + back)
        return [
            [
                inside[k][r] + pf[r] * carried[k] + pb[r] * carried[count + k]
                for r in range(E)
            ]
            for k in range(count)
        ]

    def apply_k(_, carry):
        sums = totals(
            [[w[k, r] * x[r] for r in range(E)] for k in range(3)]
            + [[g[r] * x[r] for r in range(E)]]
        )
        slot_x = [sx[r] for r in range(S)]
        cross_x = pick([slot_x], [crow[r] for r in range(E)], [clane[r] for r in range(E)])[0]
        slot_sum = pick([sums[3]], [srow[r] for r in range(S)], [slane[r] for r in range(S)])[0]
        z = [
            m[r] * (w[0, r] * sums[0][r] + w[1, r] * sums[1][r] + w[2, r] * sums[2][r] + g[r] * cross_x[r])
            for r in range(E)
        ]
        slot_z = [sm[r] * (slot_sum[r] + sww[r] * slot_x[r]) for r in range(S)]
        slot_twin = swap(slot_z)
        for r in range(S):
            new = slot_x[r] - (slot_z[r] + slot_twin[r])
            sx[r] = new
            sxt[r] = sxt[r] + new
        z_twin = pick([z], [prow[r] for r in range(E)], [plane[r] for r in range(E)])[0]
        for r in range(E):
            new = x[r] - (z[r] + z_twin[r])
            x[r] = new
            xt[r] = xt[r] + new
        return carry

    def solve(index, carry):
        for r in range(E):
            xt[r] = x[r]
        for r in range(S):
            sxt[r] = sx[r]
        lax.fori_loop(0, ORDER, apply_k, 0)
        sums = totals([[w[k, r] * xt[r] for r in range(E)] for k in range(3)])
        slot_xt = [sxt[r] for r in range(S)]
        cross_x = pick([slot_xt], [crow[r] for r in range(E)], [clane[r] for r in range(E)])[0]
        slot_sum = pick(sums, [srow[r] for r in range(S)], [slane[r] for r in range(S)])
        for k in range(3):
            for r in range(E):
                delta[k, r] = delta[k, r] - m[r] * (sums[k][r] + wc[k, r] * cross_x[r])
            for r in range(S):
                sdelta[k, r] = sdelta[k, r] - sm[r] * (slot_sum[k][r] + sw[k, r] * slot_xt[r])

        @pl.when(index < ITER)
        def _():
            def lengthening(gap, far, s):
                target = jnp.sqrt(2.0 * far * far - dot3(gap, gap))
                return s * (far - target)

            here = [[delta[k, r] for r in range(E)] for k in range(3)]
            there = pick(here, [prow[r] for r in range(E)], [plane[r] for r in range(E)])
            for r in range(E):
                gap = [d[k, r] + (here[k][r] - there[k][r]) for k in range(3)]
                x[r] = lengthening(gap, length[r], scale[r])
            here = [[sdelta[k, r] for r in range(S)] for k in range(3)]
            there = [swap(part) for part in here]
            for r in range(S):
                gap = [sd[k, r] + (here[k][r] - there[k][r]) for k in range(3)]
                sx[r] = lengthening(gap, slength[r], sscale[r])

        return carry

    lax.fori_loop(0, ITER + 1, solve, 0)

    me = lax.axis_index("dom")

    def own_row(ref, k):
        return lambda r: jnp.broadcast_to(ref[k, r, pl.ds(me, 1), :], (8, 128))

    places = [local[pl.ds(8 * q, 8), :].astype(i32) for q in range(4)]
    rows, lanes = [p >> 7 for p in places], [p & 127 for p in places]
    inner = gather_rows([own_row(delta, k) for k in range(3)], E, rows[:2], lanes[:2])
    outer = gather_rows([own_row(sdelta, k) for k in range(3)], S, rows[2:], lanes[2:])
    for q in range(2):
        for k in range(3):
            xt[3 * q + k] = jnp.where(rows[q] >= 0, inner[q][k], outer[q][k])
    for k in range(3):
        for r in range(16):
            at = pl.ds(128 * r, 128)
            change = xt[3 * (r // 8) + k, pl.ds(r % 8, 1), :]
            out[pl.ds(k, 1), at] = vel[pl.ds(k, 1), at] + change / time_step


CHUNKS = ((0, 72), (72, 72), (144, 64), (208, 64))


def share(block, out, send, recv, local_sem):
    me = lax.axis_index("dom")
    count = out.shape[0]
    last = count // 2 - 1
    z, core = me // 2, me % 2
    partner, up, down = 2 * z + 1 - core, me + 2, me - 2

    barrier = pltpu.get_barrier_semaphore()

    def greet(target):
        pl.semaphore_signal(
            barrier, inc=1, device_id={"dom": target}, device_id_type=pl.DeviceIdType.MESH
        )

    greet(partner)

    @pl.when(z < last)
    def _():
        greet(up)

    @pl.when(z > 0)
    def _():
        greet(down)

    peers = 1 + jnp.where(z < last, 1, 0) + jnp.where(z > 0, 1, 0)
    pl.semaphore_wait(barrier, peers)

    def copy(origin, source, k, target, sem):
        rows = pl.ds(*CHUNKS[k])
        return pltpu.make_async_remote_copy(
            src_ref=origin.at[rows],
            dst_ref=out.at[source, rows],
            send_sem=send.at[sem, k],
            recv_sem=recv.at[source, k],
            device_id={"dom": target},
            device_id_type=pl.DeviceIdType.MESH,
        )

    here = pltpu.make_async_copy(block, out.at[me], local_sem)
    here.start()
    sent = []

    def push(when, origin, source, k, target, sem):
        sent.append((when, origin, source, k, target, sem))

        @pl.when(when)
        def _():
            copy(origin, source, k, target, sem).start()

    for k in range(len(CHUNKS)):
        push(z < last, block, me, k, up, 0)
        push(z > 0, block, me, k, down, 1)
        push(z >= 0, block, me, k, partner, 2)
    for away in range(1, last + 1):
        for k in range(len(CHUNKS)):
            for side, arrives, source, onward, target in (
                (0, z >= away, me - 2 * away, z < last, up),
                (1, z + away <= last, me + 2 * away, z > 0, down),
            ):
                sem = 3 + 4 * (away - 1) + 2 * side

                @pl.when(arrives)
                def _(source=source, k=k):
                    copy(out.at[source], source, k, partner, 0).wait_recv()

                if away < last:
                    push(arrives & onward, out.at[source], source, k, target, sem)
                push(arrives, out.at[source], source, k, partner, sem + 1)
    for k in range(len(CHUNKS)):
        for chip in range(last + 1):
            source = 2 * chip + 1 - core
            copy(out.at[source], source, k, partner, 0).wait_recv()
    for when, origin, source, k, target, sem in sent:

        @pl.when(when)
        def _(origin=origin, source=source, k=k, target=target, sem=sem):
            copy(origin, source, k, target, sem).wait_send()

    here.wait()


def on_device(
    protein_pos, protein_vel, inv_mass, bond_atoms, left_atoms, right_atoms, water_pos, water_vel
):
    vmem = pl.BlockSpec(memory_space=pltpu.VMEM)
    block, local, water_velocity = pl.pallas_call(
        prepare,
        out_shape=(
            jax.ShapeDtypeStruct((ROWS, 128), f32),
            jax.ShapeDtypeStruct((32, 128), f32),
            jax.ShapeDtypeStruct(water_pos.shape, f32),
        ),
        in_specs=[vmem] * 8,
        out_specs=(vmem,) * 3,
        scratch_shapes=[
            pltpu.VMEM((7, 16, 128), f32),
            pltpu.VMEM((32, 128), i32),
            pltpu.VMEM((24, 128), i32),
            pltpu.VMEM((24, 128), i32),
            pltpu.VMEM((32, 128), i32),
            pltpu.VMEM((8, 128), i32),
            pltpu.VMEM((18, 8, 128), f32),
        ],
        name="prepare",
    )(
        protein_pos,
        protein_vel,
        inv_mass.reshape(16, 128),
        bond_atoms,
        left_atoms.reshape(3, 128),
        right_atoms.reshape(3, 128),
        water_pos,
        water_vel,
    )
    count = lax.axis_size("dom")
    data = pl.pallas_call(
        share,
        out_shape=jax.ShapeDtypeStruct((count, ROWS, 128), f32),
        in_specs=[vmem],
        out_specs=vmem,
        scratch_shapes=[
            pltpu.SemaphoreType.DMA((4 * count // 2, len(CHUNKS))),
            pltpu.SemaphoreType.DMA((count, len(CHUNKS))),
            pltpu.SemaphoreType.DMA,
        ],
        compiler_params=pltpu.CompilerParams(collective_id=0, has_side_effects=True),
        name="share",
    )(block)
    real = [(3, E), (E,), (E,)]
    scratch = [
        ((3, E), f32), ((E,), f32), ((E,), f32),
        ((E,), i32), ((E,), i32), ((E,), i32), ((E,), i32),
        ((E,), f32), ((E,), f32), ((E,), f32),
        ((E,), f32), ((E,), f32),
        ((3, E), f32), ((3, E), f32), ((E,), f32), ((E,), f32), ((3, E), f32),
        ((3, S), f32), ((S,), f32), ((S,), i32), ((S,), i32), ((S,), f32),
        ((S,), f32), ((S,), f32), ((3, S), f32), ((S,), f32), ((S,), f32), ((3, S), f32),
    ]
    protein_velocity = pl.pallas_call(
        rounds,
        out_shape=jax.ShapeDtypeStruct(protein_vel.shape, f32),
        in_specs=[vmem] * 3,
        out_specs=vmem,
        scratch_shapes=[pltpu.VMEM(shape + (8, 128), kind) for shape, kind in scratch],
        name="rounds",
    )(data, local, protein_vel)
    return (protein_velocity, water_velocity)


def solution(mesh):
    in_specs = (
        P(None, ("rep", "dom")),
        P(None, ("rep", "dom")),
        P(("rep", "dom")),
        P(None, ("rep", "dom")),
        P(("rep", "dom")),
        P(("rep", "dom")),
        P(None, ("rep", "dom")),
        P(None, ("rep", "dom")),
    )
    out_specs = (P(None, ("rep", "dom")), P(None, ("rep", "dom")))
    return jax.shard_map(
        on_device, mesh=mesh, in_specs=in_specs, out_specs=out_specs, check_vma=False
    )
```

```python
import math

import jax
import jax.numpy as jnp
from jax import lax
from jax.experimental import pallas as pl
from jax.experimental.pallas import tpu as pltpu
from jax.sharding import PartitionSpec as P

ORDER = 4
ITER = 2

time_step = 0.002
mass_oxygen = 15.9994
mass_hydrogen = 1.008
oxygen_hydrogen = 0.09572
hydrogen_pair = 0.15139
total_mass = mass_oxygen + 2.0 * mass_hydrogen
half_pair = 0.5 * hydrogen_pair
water_height = math.sqrt(oxygen_hydrogen * oxygen_hydrogen - half_pair * half_pair)
oxygen_reach = 2.0 * mass_hydrogen * water_height / total_mass
hydrogen_reach = water_height - oxygen_reach

E = 20
S = 6
DIFF, DVEL, SCALE, MASS, PIDX, CONT, CIDX = 0, 3 * E, 6 * E, 7 * E, 8 * E, 9 * E, 10 * E
SPOS = 11 * E
SVEL, SMASS, SIDX = SPOS + 3 * S, SPOS + 6 * S, SPOS + 7 * S
ROWS = 272
f32, i32 = jnp.float32, jnp.int32


def take(table, lanes):
    return jnp.take_along_axis(table, lanes, axis=1, mode="promise_in_bounds")


def cross3(a, b):
    return (
        a[1] * b[2] - a[2] * b[1],
        a[2] * b[0] - a[0] * b[2],
        a[0] * b[1] - a[1] * b[0],
    )


def dot3(a, b):
    return a[0] * b[0] + a[1] * b[1] + a[2] * b[2]


def settle(old, vel):
    old_b = [old[3 + k] - old[k] for k in range(3)]
    old_c = [old[6 + k] - old[k] for k in range(3)]
    new_a = [time_step * vel[k] for k in range(3)]
    new_b = [old_b[k] + time_step * vel[3 + k] for k in range(3)]
    new_c = [old_c[k] + time_step * vel[6 + k] for k in range(3)]
    center = [
        (mass_oxygen * new_a[k] + mass_hydrogen * (new_b[k] + new_c[k])) / total_mass
        for k in range(3)
    ]
    rel_a = [new_a[k] - center[k] for k in range(3)]
    rel_b = [new_b[k] - center[k] for k in range(3)]
    rel_c = [new_c[k] - center[k] for k in range(3)]
    normal = cross3(old_b, old_c)
    side = cross3(rel_a, normal)
    upward = cross3(normal, side)

    def norm(vec):
        size = jnp.sqrt(dot3(vec, vec))
        return [part / size for part in vec]

    axis_z, axis_x, axis_y = norm(normal), norm(side), norm(upward)
    oldb_x, oldb_y = dot3(axis_x, old_b), dot3(axis_y, old_b)
    oldc_x, oldc_y = dot3(axis_x, old_c), dot3(axis_y, old_c)
    newa_z = dot3(axis_z, rel_a)
    newb_x, newb_y, newb_z = dot3(axis_x, rel_b), dot3(axis_y, rel_b), dot3(axis_z, rel_b)
    newc_x, newc_y, newc_z = dot3(axis_x, rel_c), dot3(axis_y, rel_c), dot3(axis_z, rel_c)
    sin_phi = newa_z / oxygen_reach
    cos_phi = jnp.sqrt(1.0 - sin_phi * sin_phi)
    sin_psi = (newb_z - newc_z) / (2.0 * half_pair * cos_phi)
    cos_psi = jnp.sqrt(1.0 - sin_psi * sin_psi)
    rest_ay = oxygen_reach * cos_phi
    rest_bx = -half_pair * cos_psi
    lowered = -hydrogen_reach * cos_phi
    tilted = half_pair * sin_psi * sin_phi
    rest_by = lowered - tilted
    rest_cy = lowered + tilted
    alpha = rest_bx * (oldb_x - oldc_x) + oldb_y * rest_by + oldc_y * rest_cy
    beta = rest_bx * (oldc_y - oldb_y) + oldb_x * rest_by + oldc_x * rest_cy
    gamma = oldb_x * newb_y - newb_x * oldb_y + oldc_x * newc_y - newc_x * oldc_y
    summed = alpha * alpha + beta * beta
    sin_theta = (alpha * gamma - beta * jnp.sqrt(summed - gamma * gamma)) / summed
    cos_theta = jnp.sqrt(1.0 - sin_theta * sin_theta)
    final_ax = -rest_ay * sin_theta
    final_ay = rest_ay * cos_theta
    final_bx = rest_bx * cos_theta - rest_by * sin_theta
    final_by = rest_bx * sin_theta + rest_by * cos_theta
    final_cx = -rest_bx * cos_theta - rest_cy * sin_theta
    final_cy = -rest_bx * sin_theta + rest_cy * cos_theta
    out = []
    for rel, along_x, along_y, along_z in (
        (rel_a, final_ax, final_ay, newa_z),
        (rel_b, final_bx, final_by, newb_z),
        (rel_c, final_cx, final_cy, newc_z),
    ):
        for k in range(3):
            out.append(axis_x[k] * along_x + axis_y[k] * along_y + axis_z[k] * along_z - rel[k])
    return [vel[k] + out[k] / time_step for k in range(9)]


def sort4(x):
    lane = lax.broadcasted_iota(i32, (8, 128), 1)
    sub = lax.broadcasted_iota(i32, (8, 128), 0)
    within = (lane << 5) | (sub << 2)
    x = list(x)
    for k in range(1, 13):
        for j in range(k - 1, -1, -1):
            if j < 2:
                for a in range(4):
                    b = a | (1 << j)
                    if a == b:
                        continue
                    low, high = jnp.minimum(x[a], x[b]), jnp.maximum(x[a], x[b])
                    if k == 12:
                        x[a], x[b] = low, high
                    elif k < 2:
                        x[a], x[b] = (low, high) if not (a >> k) & 1 else (high, low)
                    else:
                        up = ((within >> k) & 1) == 0
                        x[a], x[b] = jnp.where(up, low, high), jnp.where(up, high, low)
                continue
            first = ((within >> j) & 1) == 0
            if k == 12:
                keep_low = first
            else:
                keep_low = ((within >> j) & 1) == ((within >> k) & 1)
            for a in range(4):
                if j < 5:
                    step = 1 << (j - 2)
                    if step == 4:
                        other = pltpu.roll(x[a], 4, 0)
                    else:
                        other = jnp.where(
                            first, pltpu.roll(x[a], 8 - step, 0), pltpu.roll(x[a], step, 0)
                        )
                else:
                    other = take(x[a], lane ^ (1 << (j - 5)))
                x[a] = jnp.where(keep_low, jnp.minimum(x[a], other), jnp.maximum(x[a], other))
    return x


def gather_rows(tables, count, rows, lanes):
    outs = []
    for row_at, lane_at in zip(rows, lanes):
        hits = [row_at == r for r in range(count)]
        got = []
        for table in tables:
            acc = jnp.zeros((8, 128), table(0).dtype)
            for r in range(count):
                acc = jnp.where(hits[r], take(table(r), lane_at), acc)
            got.append(acc)
        outs.append(got)
    return outs


def row_of(ref, *base):
    def read(r):
        return jnp.broadcast_to(ref[base + (pl.ds(r, 1),)] if base else ref[pl.ds(r, 1), :], (8, 128))

    return read


def prepare(
    pos, vel, mass, bonds, left, right, block, local, table, ends, keys, atoms, before, slots,
):
    lane = lax.broadcasted_iota(i32, (8, 128), 1)
    sub = lax.broadcasted_iota(i32, (8, 128), 0)
    for r in range(16):
        at = pl.ds(128 * r, 128)
        for k in range(3):
            table[k, pl.ds(r, 1)] = pos[pl.ds(k, 1), at]
            table[3 + k, pl.ds(r, 1)] = vel[pl.ds(k, 1), at]
        table[6, pl.ds(r, 1)] = mass[pl.ds(r, 1), :]
    for half in range(2):
        ends[pl.ds(16 * half + 8, 8), :] = jnp.full((8, 128), 2048, i32)
        for r in range(10):
            ends[pl.ds(16 * half + r, 1), :] = bonds[pl.ds(half, 1), pl.ds(128 * r, 128)]
    slots[...] = jnp.zeros((8, 128), i32)
    for r in range(3):
        slots[pl.ds(r, 1), :] = right[pl.ds(r, 1), :]
        slots[pl.ds(3 + r, 1), :] = left[pl.ds(r, 1), :]

    start = []
    for q in range(4):
        at = sub + 8 * q
        start.append((ends[pl.ds(8 * q, 8), :] << 12) | (at << 7) | lane)
    done = sort4(start)
    for q in range(4):
        before[pl.ds(8 * q, 8), :] = done[q]
    rows, lanes = [], []
    for q in range(3):
        n = jnp.minimum(lane * E + sub + 8 * q, 4095)
        rows.append(((n & 3) << 3) | ((n >> 2) & 7))
        lanes.append(n >> 5)
    key = [g[0] for g in gather_rows([row_of(before)], 32, rows, lanes)]
    for q in range(3):
        keys[pl.ds(8 * q, 8), :] = key[q]
    atom = [k >> 12 for k in key]
    twin = [(k & 4095) ^ 2048 for k in key]
    other = [
        g[0]
        for g in gather_rows([row_of(ends)], 26, [t >> 7 for t in twin], [t & 127 for t in twin])
    ]

    slot_atom = slots[...]
    own_atom = [(sub + 8 * q) * 128 + lane for q in range(2)]
    queries = [(other[q] << 12) | twin[q] for q in range(3)]
    queries += [(a << 12) | 4095 for a in [slot_atom] + own_atom]
    leaders = jnp.broadcast_to(keys[pl.ds(0, 1), :], (8, 128))
    found_row, found_lane, found_key = [], [], []
    for query in queries:
        low = jnp.zeros((8, 128), i32)
        for bit in (64, 32, 16, 8, 4, 2, 1):
            low = jnp.where(take(leaders, low + bit) <= query, low + bit, low)
        count = jnp.full((8, 128), -1, i32)
        best = jnp.full((8, 128), -1, i32)
        for r in range(E):
            seen = take(jnp.broadcast_to(keys[pl.ds(r, 1), :], (8, 128)), low)
            less = seen <= query
            count = jnp.where(less, count + 1, count)
            best = jnp.where(less, seen, best)
        found_row.append(count)
        found_lane.append(low)
        found_key.append(best)
    places = [found_row[q] * 128 + found_lane[q] for q in range(6)]
    slot_place = jnp.where((found_key[3] >> 12) == slot_atom, places[3], -1)
    for q in range(2):
        place = jnp.where((found_key[4 + q] >> 12) == own_atom[q], places[4 + q], -1)
        local[pl.ds(8 * q, 8), :] = place.astype(f32)

    high = lax.broadcasted_iota(i32, (16, 128), 0)
    code = lax.broadcasted_iota(i32, (16, 128), 1) + 1
    low_of = lax.broadcasted_iota(i32, (128, 128), 0)
    which = jnp.zeros((32, 128), f32)
    for r in range(S):
        here = slots[pl.ds(r, 1), :]
        mine = jnp.broadcast_to(here >> 7, (16, 128)) == high
        left_side = jnp.concatenate(
            [jnp.where(mine, code, 0).astype(f32), jnp.where(mine, r + 1, 0).astype(f32)], axis=0
        )
        right_side = jnp.where(jnp.broadcast_to(here & 127, (128, 128)) == low_of, 1.0, 0.0)
        which = which + lax.dot_general(
            left_side.astype(jnp.bfloat16),
            right_side.astype(jnp.bfloat16),
            (((1,), (1,)), ((), ())),
            preferred_element_type=f32,
        )
    local[pl.ds(16, 16), :] = jnp.where(
        which[0:16] > 0.0, which[16:32] * 128.0 + which[0:16] - 129.0, -1.0
    )

    for q in range(3):
        atoms[pl.ds(8 * q, 8), :] = atom[q]
    before[pl.ds(0, 1), :] = pltpu.roll(atoms[pl.ds(E - 1, 1), :], 1, 1)
    before[pl.ds(1, E - 1), :] = atoms[pl.ds(0, E - 1), :]
    own_rows, own_lanes = [a >> 7 for a in atom], [a & 127 for a in atom]
    tables = [row_of(table, k) for k in range(7)] + [row_of(local.at[pl.ds(16, 16)])]
    own = gather_rows(tables, 16, own_rows, own_lanes)
    far = gather_rows(tables[:7], 16, [a >> 7 for a in other], [a & 127 for a in other])
    for q in range(3):
        size = min(8, E - 8 * q)

        def put(base, value):
            block[pl.ds(base + 8 * q, size), :] = value[0:size]

        for k in range(3):
            put(DIFF + E * k, own[q][k] - far[q][k])
            put(DVEL + E * k, own[q][3 + k] - far[q][3 + k])
        put(SCALE, 1.0 / jnp.sqrt(own[q][6] + far[q][6]))
        put(MASS, own[q][6])
        put(PIDX, places[q].astype(f32))
        same = before[pl.ds(8 * q, 8), :] == atom[q]
        if q == 0:
            same = same & ((lane > 0) | (sub > 0))
        put(CONT, jnp.where(same, 1.0, 0.0))
        put(CIDX, own[q][7])
    at_slots = gather_rows(tables[:7], 16, [slot_atom >> 7], [slot_atom & 127])[0]
    for k in range(7):
        block[pl.ds(SPOS + S * k, S), :] = at_slots[k][0:S]
    block[pl.ds(SIDX, S), :] = slot_place.astype(f32)[0:S]
    block[pl.ds(SIDX + S, ROWS - SIDX - S), :] = jnp.zeros((ROWS - SIDX - S, 128), f32)


def waters(wpos, wvel, wout, water):
    for k in range(9):
        for r in range(8):
            water[k, pl.ds(r, 1)] = wpos[pl.ds(k, 1), pl.ds(128 * r, 128)]
            water[9 + k, pl.ds(r, 1)] = wvel[pl.ds(k, 1), pl.ds(128 * r, 128)]
    new = settle([water[k] for k in range(9)], [water[9 + k] for k in range(9)])
    for k in range(9):
        water[k] = new[k]
        for r in range(8):
            wout[pl.ds(k, 1), pl.ds(128 * r, 128)] = water[k, pl.ds(r, 1)]


def pick(tables, rows, lanes):
    outs = [[] for _ in tables]
    for row_at, lane_at in zip(rows, lanes):
        hits = [row_at == r for r in range(len(tables[0]))]
        for out, table in zip(outs, tables):
            acc = jnp.zeros((8, 128), f32)
            for hit, part in zip(hits, table):
                acc = jnp.where(hit, take(part, lane_at), acc)
            out.append(acc)
    return outs


def swap(slots):
    back = [pltpu.roll(part, 7, 0) for part in slots[3:6]]
    ahead = [pltpu.roll(part, 1, 0) for part in slots[0:3]]
    return back + ahead


def rounds(
    data, local, vel_in, water, out, water_out,
    w, g, m, prow, plane, crow, clane, cont, pf, pb, x, xt, wc, d, length, scale, delta,
    sw, sm, srow, slane, sww, sx, sxt, sd, slength, sscale, sdelta, vel, vel_sem, water_sem,
):
    load = pltpu.make_async_copy(vel_in, vel, vel_sem)
    load.start()
    passed = pltpu.make_async_copy(water, water_out, water_sem)
    passed.start()

    def rows_at(base, count):
        return [data[:, base + r, :] for r in range(count)]

    for base, row_ref, lane_ref, count in ((PIDX, prow, plane, E), (CIDX, crow, clane, E), (SIDX, srow, slane, S)):
        for r in range(count):
            value = data[:, base + r, :].astype(i32)
            row_ref[r] = value >> 7
            lane_ref[r] = value & 127
    keep = rows_at(CONT, E)
    run = jnp.ones((8, 128), f32)
    for r in range(E):
        cont[r] = keep[r]
        if r > 0:
            run = run * keep[r]
        pf[r] = run
    whole = run
    run = jnp.ones((8, 128), f32)
    for r in range(E - 1, -1, -1):
        pb[r] = run
        run = run * keep[r]
    extra = jnp.max(jnp.sum(whole, axis=1, keepdims=True)).astype(i32)
    opens = keep[0]
    closes = pltpu.roll(opens, 127, 1)

    def geometry(diff, dvel, s):
        far = jnp.sqrt(dot3(diff, diff))
        ratio = s / far
        weight = [ratio * part for part in diff]
        moved = [diff[k] + time_step * dvel[k] for k in range(3)]
        return far, weight, moved, time_step * dot3(weight, dvel)

    own = [rows_at(SPOS + S * k, S) for k in range(7)]
    twin = [swap(part) for part in own]
    for r in range(S):
        diff = [own[k][r] - twin[k][r] for k in range(3)]
        dvel = [own[3 + k][r] - twin[3 + k][r] for k in range(3)]
        s = 1.0 / jnp.sqrt(own[6][r] + twin[6][r])
        far, weight, moved, first = geometry(diff, dvel, s)
        for k in range(3):
            sw[k, r] = weight[k]
            sd[k, r] = moved[k]
            sdelta[k, r] = jnp.zeros((8, 128), f32)
        sm[r] = own[6][r]
        sww[r] = dot3(weight, weight)
        slength[r] = far
        sscale[r] = s
        sx[r] = first
    near = pick(
        [[sw[k, r] for r in range(S)] for k in range(3)],
        [crow[r] for r in range(E)],
        [clane[r] for r in range(E)],
    )
    for r in range(E):
        diff = [data[:, DIFF + E * k + r, :] for k in range(3)]
        dvel = [data[:, DVEL + E * k + r, :] for k in range(3)]
        s = data[:, SCALE + r, :]
        far, weight, moved, first = geometry(diff, dvel, s)
        for k in range(3):
            w[k, r] = weight[k]
            d[k, r] = moved[k]
            wc[k, r] = near[k][r]
            delta[k, r] = jnp.zeros((8, 128), f32)
        g[r] = dot3(weight, [near[k][r] for k in range(3)])
        m[r] = data[:, MASS + r, :]
        length[r] = far
        scale[r] = s
        x[r] = first

    def totals(parts):
        count = len(parts)
        inside = []
        for part in parts:
            acc = part[0]
            fwd = [acc]
            for r in range(1, E):
                acc = part[r] + cont[r] * acc
                fwd.append(acc)
            for r in range(E - 2, -1, -1):
                fwd[r] = jnp.where(cont[r + 1] > 0.0, fwd[r + 1], fwd[r])
            inside.append(fwd)
        ahead = tuple(opens * pltpu.roll(part[E - 1], 1, 1) for part in inside)
        back = tuple(closes * pltpu.roll(part[0], 127, 1) for part in inside)

        def spread(_, now):
            ahead_now, back_now = now[:count], now[count:]
            new = [ahead[k] + opens * pltpu.roll(whole * ahead_now[k], 1, 1) for k in range(count)]
            new += [back[k] + closes * pltpu.roll(whole * back_now[k], 127, 1) for k in range(count)]
            return tuple(new)

        carried = lax.fori_loop(0, extra, spread, ahead + back)
        return [
            [
                inside[k][r] + pf[r] * carried[k] + pb[r] * carried[count + k]
                for r in range(E)
            ]
            for k in range(count)
        ]

    def apply_k(_, carry):
        sums = totals(
            [[w[k, r] * x[r] for r in range(E)] for k in range(3)]
            + [[g[r] * x[r] for r in range(E)]]
        )
        slot_x = [sx[r] for r in range(S)]
        cross_x = pick([slot_x], [crow[r] for r in range(E)], [clane[r] for r in range(E)])[0]
        slot_sum = pick([sums[3]], [srow[r] for r in range(S)], [slane[r] for r in range(S)])[0]
        z = [
            m[r] * (w[0, r] * sums[0][r] + w[1, r] * sums[1][r] + w[2, r] * sums[2][r] + g[r] * cross_x[r])
            for r in range(E)
        ]
        slot_z = [sm[r] * (slot_sum[r] + sww[r] * slot_x[r]) for r in range(S)]
        slot_twin = swap(slot_z)
        for r in range(S):
            new = slot_x[r] - (slot_z[r] + slot_twin[r])
            sx[r] = new
            sxt[r] = sxt[r] + new
        z_twin = pick([z], [prow[r] for r in range(E)], [plane[r] for r in range(E)])[0]
        for r in range(E):
            new = x[r] - (z[r] + z_twin[r])
            x[r] = new
            xt[r] = xt[r] + new
        return carry

    def solve(index, carry):
        for r in range(E):
            xt[r] = x[r]
        for r in range(S):
            sxt[r] = sx[r]
        lax.fori_loop(0, ORDER, apply_k, 0)
        sums = totals([[w[k, r] * xt[r] for r in range(E)] for k in range(3)])
        slot_xt = [sxt[r] for r in range(S)]
        cross_x = pick([slot_xt], [crow[r] for r in range(E)], [clane[r] for r in range(E)])[0]
        slot_sum = pick(sums, [srow[r] for r in range(S)], [slane[r] for r in range(S)])
        for k in range(3):
            for r in range(E):
                delta[k, r] = delta[k, r] - m[r] * (sums[k][r] + wc[k, r] * cross_x[r])
            for r in range(S):
                sdelta[k, r] = sdelta[k, r] - sm[r] * (slot_sum[k][r] + sw[k, r] * slot_xt[r])

        @pl.when(index < ITER)
        def _():
            def lengthening(gap, far, s):
                target = jnp.sqrt(2.0 * far * far - dot3(gap, gap))
                return s * (far - target)

            here = [[delta[k, r] for r in range(E)] for k in range(3)]
            there = pick(here, [prow[r] for r in range(E)], [plane[r] for r in range(E)])
            for r in range(E):
                gap = [d[k, r] + (here[k][r] - there[k][r]) for k in range(3)]
                x[r] = lengthening(gap, length[r], scale[r])
            here = [[sdelta[k, r] for r in range(S)] for k in range(3)]
            there = [swap(part) for part in here]
            for r in range(S):
                gap = [sd[k, r] + (here[k][r] - there[k][r]) for k in range(3)]
                sx[r] = lengthening(gap, slength[r], sscale[r])

        return carry

    lax.fori_loop(0, ITER + 1, solve, 0)

    me = lax.axis_index("dom")

    def own_row(ref, k):
        return lambda r: jnp.broadcast_to(ref[k, r, pl.ds(me, 1), :], (8, 128))

    load.wait()
    places = [local[pl.ds(8 * q, 8), :].astype(i32) for q in range(4)]
    rows, lanes = [p >> 7 for p in places], [p & 127 for p in places]
    inner = gather_rows([own_row(delta, k) for k in range(3)], E, rows[:2], lanes[:2])
    outer = gather_rows([own_row(sdelta, k) for k in range(3)], S, rows[2:], lanes[2:])
    for q in range(2):
        for k in range(3):
            xt[3 * q + k] = jnp.where(rows[q] >= 0, inner[q][k], outer[q][k])
    for k in range(3):
        for r in range(16):
            at = pl.ds(128 * r, 128)
            change = xt[3 * (r // 8) + k, pl.ds(r % 8, 1), :]
            out[pl.ds(k, 1), at] = vel[pl.ds(k, 1), at] + change / time_step
    passed.wait()


CHUNKS = ((0, 72), (72, 72), (144, 64), (208, 64))


def share(
    pos_in, vel_in, mass_in, bonds_in, left_in, right_in, wpos_in, wvel_in, out, local, wout,
    pos, vel, mass, bonds, left, right, wpos, wvel,
    block, table, ends, keys, atoms, before, slots, water, send, recv, local_sem, load_sem,
):
    me = lax.axis_index("dom")
    count = out.shape[0]
    last = count // 2 - 1
    z, core = me // 2, me % 2
    partner, up, down = 2 * z + 1 - core, me + 2, me - 2

    loads = [
        pltpu.make_async_copy(origin, target, load_sem.at[k])
        for k, (origin, target) in enumerate(
            (
                (bonds_in, bonds), (pos_in, pos), (vel_in, vel), (mass_in, mass),
                (left_in, left), (right_in, right), (wpos_in, wpos), (wvel_in, wvel),
            )
        )
    ]
    for load in loads:
        load.start()
    barrier = pltpu.get_barrier_semaphore()

    def greet(target):
        pl.semaphore_signal(
            barrier, inc=1, device_id={"dom": target}, device_id_type=pl.DeviceIdType.MESH
        )

    greet(partner)

    @pl.when(z < last)
    def _():
        greet(up)

    @pl.when(z > 0)
    def _():
        greet(down)

    peers = 1 + jnp.where(z < last, 1, 0) + jnp.where(z > 0, 1, 0)
    for load in loads[:6]:
        load.wait()
    prepare(
        pos, vel, mass, bonds, left, right, block, local, table, ends, keys, atoms, before, slots
    )
    pl.semaphore_wait(barrier, peers)

    def copy(origin, source, k, target, sem):
        rows = pl.ds(*CHUNKS[k])
        return pltpu.make_async_remote_copy(
            src_ref=origin.at[rows],
            dst_ref=out.at[source, rows],
            send_sem=send.at[sem, k],
            recv_sem=recv.at[source, k],
            device_id={"dom": target},
            device_id_type=pl.DeviceIdType.MESH,
        )

    here = pltpu.make_async_copy(block, out.at[me], local_sem)
    here.start()
    sent = []

    def push(when, origin, source, k, target, sem):
        sent.append((when, origin, source, k, target, sem))

        @pl.when(when)
        def _():
            copy(origin, source, k, target, sem).start()

    for k in range(len(CHUNKS)):
        push(z < last, block, me, k, up, 0)
        push(z > 0, block, me, k, down, 1)
        push(z >= 0, block, me, k, partner, 2)
    for load in loads[6:]:
        load.wait()
    waters(wpos, wvel, wout, water)
    for away in range(1, last + 1):
        for k in range(len(CHUNKS)):
            for side, arrives, source, onward, target in (
                (0, z >= away, me - 2 * away, z < last, up),
                (1, z + away <= last, me + 2 * away, z > 0, down),
            ):
                sem = 3 + 4 * (away - 1) + 2 * side

                @pl.when(arrives)
                def _(source=source, k=k):
                    copy(out.at[source], source, k, partner, 0).wait_recv()

                if away < last:
                    push(arrives & onward, out.at[source], source, k, target, sem)
                push(arrives, out.at[source], source, k, partner, sem + 1)
    for k in range(len(CHUNKS)):
        for chip in range(last + 1):
            source = 2 * chip + 1 - core
            copy(out.at[source], source, k, partner, 0).wait_recv()
    for when, origin, source, k, target, sem in sent:

        @pl.when(when)
        def _(origin=origin, source=source, k=k, target=target, sem=sem):
            copy(origin, source, k, target, sem).wait_send()

    here.wait()


def on_device(
    protein_pos, protein_vel, inv_mass, bond_atoms, left_atoms, right_atoms, water_pos, water_vel
):
    vmem = pl.BlockSpec(memory_space=pltpu.VMEM)
    hbm = pl.BlockSpec(memory_space=pltpu.HBM)
    count = lax.axis_size("dom")
    data, local, water_velocity = pl.pallas_call(
        share,
        out_shape=(
            jax.ShapeDtypeStruct((count, ROWS, 128), f32),
            jax.ShapeDtypeStruct((32, 128), f32),
            jax.ShapeDtypeStruct(water_pos.shape, f32),
        ),
        in_specs=[hbm] * 8,
        out_specs=(vmem,) * 3,
        scratch_shapes=[
            pltpu.VMEM(protein_pos.shape, f32),
            pltpu.VMEM(protein_vel.shape, f32),
            pltpu.VMEM((16, 128), f32),
            pltpu.VMEM(bond_atoms.shape, i32),
            pltpu.VMEM((3, 128), i32),
            pltpu.VMEM((3, 128), i32),
            pltpu.VMEM(water_pos.shape, f32),
            pltpu.VMEM(water_vel.shape, f32),
            pltpu.VMEM((ROWS, 128), f32),
            pltpu.VMEM((7, 16, 128), f32),
            pltpu.VMEM((32, 128), i32),
            pltpu.VMEM((24, 128), i32),
            pltpu.VMEM((24, 128), i32),
            pltpu.VMEM((32, 128), i32),
            pltpu.VMEM((8, 128), i32),
            pltpu.VMEM((18, 8, 128), f32),
            pltpu.SemaphoreType.DMA((4 * count // 2, len(CHUNKS))),
            pltpu.SemaphoreType.DMA((count, len(CHUNKS))),
            pltpu.SemaphoreType.DMA,
            pltpu.SemaphoreType.DMA((8,)),
        ],
        compiler_params=pltpu.CompilerParams(
            collective_id=0, has_side_effects=True, vmem_limit_bytes=16 * 2**20
        ),
        name="share",
    )(
        *(
            pltpu.with_memory_space_constraint(value, pltpu.HBM)
            for value in (
                protein_pos,
                protein_vel,
                inv_mass.reshape(16, 128),
                bond_atoms,
                left_atoms.reshape(3, 128),
                right_atoms.reshape(3, 128),
                water_pos,
                water_vel,
            )
        )
    )
    scratch = [
        ((3, E), f32), ((E,), f32), ((E,), f32),
        ((E,), i32), ((E,), i32), ((E,), i32), ((E,), i32),
        ((E,), f32), ((E,), f32), ((E,), f32),
        ((E,), f32), ((E,), f32),
        ((3, E), f32), ((3, E), f32), ((E,), f32), ((E,), f32), ((3, E), f32),
        ((3, S), f32), ((S,), f32), ((S,), i32), ((S,), i32), ((S,), f32),
        ((S,), f32), ((S,), f32), ((3, S), f32), ((S,), f32), ((S,), f32), ((3, S), f32),
    ]
    protein_velocity, water_velocity = pl.pallas_call(
        rounds,
        out_shape=(
            jax.ShapeDtypeStruct(protein_vel.shape, f32),
            jax.ShapeDtypeStruct(water_vel.shape, f32),
        ),
        in_specs=[vmem, vmem, hbm, vmem],
        out_specs=(vmem, hbm),
        scratch_shapes=[pltpu.VMEM(shape + (8, 128), kind) for shape, kind in scratch]
        + [pltpu.VMEM(protein_vel.shape, f32), pltpu.SemaphoreType.DMA, pltpu.SemaphoreType.DMA],
        compiler_params=pltpu.CompilerParams(vmem_limit_bytes=16 * 2**20),
        name="rounds",
    )(data, local, pltpu.with_memory_space_constraint(protein_vel, pltpu.HBM), water_velocity)
    return (protein_velocity, water_velocity)


def solution(mesh):
    in_specs = (
        P(None, ("rep", "dom")),
        P(None, ("rep", "dom")),
        P(("rep", "dom")),
        P(None, ("rep", "dom")),
        P(("rep", "dom")),
        P(("rep", "dom")),
        P(None, ("rep", "dom")),
        P(None, ("rep", "dom")),
    )
    out_specs = (P(None, ("rep", "dom")), P(None, ("rep", "dom")))
    return jax.shard_map(
        on_device, mesh=mesh, in_specs=in_specs, out_specs=out_specs, check_vma=False
    )
```

```python
import math

import jax
import jax.numpy as jnp
from jax import lax
from jax.experimental import pallas as pl
from jax.experimental.pallas import tpu as pltpu
from jax.sharding import PartitionSpec as P

ORDER = 4
ITER = 2

time_step = 0.002
mass_oxygen = 15.9994
mass_hydrogen = 1.008
oxygen_hydrogen = 0.09572
hydrogen_pair = 0.15139
total_mass = mass_oxygen + 2.0 * mass_hydrogen
half_pair = 0.5 * hydrogen_pair
water_height = math.sqrt(oxygen_hydrogen * oxygen_hydrogen - half_pair * half_pair)
oxygen_reach = 2.0 * mass_hydrogen * water_height / total_mass
hydrogen_reach = water_height - oxygen_reach

B = 10
S = 6
DIFF, DVEL, SCALE, SPOS = 0, 3 * B, 6 * B, 7 * B
SVEL, SMASS = SPOS + 3 * S, SPOS + 6 * S
EARLY = SPOS + 7 * S
E = 20
MASS, PIDX, CONT, CIDX, HIDX = EARLY, EARLY + E, EARLY + 2 * E, EARLY + 3 * E, EARLY + 4 * E
SIDX = EARLY + 5 * E
ROWS = 224
f32, i32 = jnp.float32, jnp.int32


def take(table, lanes):
    return jnp.take_along_axis(table, lanes, axis=1, mode="promise_in_bounds")


def cross3(a, b):
    return (
        a[1] * b[2] - a[2] * b[1],
        a[2] * b[0] - a[0] * b[2],
        a[0] * b[1] - a[1] * b[0],
    )


def dot3(a, b):
    return a[0] * b[0] + a[1] * b[1] + a[2] * b[2]


def settle(old, vel):
    old_b = [old[3 + k] - old[k] for k in range(3)]
    old_c = [old[6 + k] - old[k] for k in range(3)]
    new_a = [time_step * vel[k] for k in range(3)]
    new_b = [old_b[k] + time_step * vel[3 + k] for k in range(3)]
    new_c = [old_c[k] + time_step * vel[6 + k] for k in range(3)]
    center = [
        (mass_oxygen * new_a[k] + mass_hydrogen * (new_b[k] + new_c[k])) / total_mass
        for k in range(3)
    ]
    rel_a = [new_a[k] - center[k] for k in range(3)]
    rel_b = [new_b[k] - center[k] for k in range(3)]
    rel_c = [new_c[k] - center[k] for k in range(3)]
    normal = cross3(old_b, old_c)
    side = cross3(rel_a, normal)
    upward = cross3(normal, side)

    def norm(vec):
        size = jnp.sqrt(dot3(vec, vec))
        return [part / size for part in vec]

    axis_z, axis_x, axis_y = norm(normal), norm(side), norm(upward)
    oldb_x, oldb_y = dot3(axis_x, old_b), dot3(axis_y, old_b)
    oldc_x, oldc_y = dot3(axis_x, old_c), dot3(axis_y, old_c)
    newa_z = dot3(axis_z, rel_a)
    newb_x, newb_y, newb_z = dot3(axis_x, rel_b), dot3(axis_y, rel_b), dot3(axis_z, rel_b)
    newc_x, newc_y, newc_z = dot3(axis_x, rel_c), dot3(axis_y, rel_c), dot3(axis_z, rel_c)
    sin_phi = newa_z / oxygen_reach
    cos_phi = jnp.sqrt(1.0 - sin_phi * sin_phi)
    sin_psi = (newb_z - newc_z) / (2.0 * half_pair * cos_phi)
    cos_psi = jnp.sqrt(1.0 - sin_psi * sin_psi)
    rest_ay = oxygen_reach * cos_phi
    rest_bx = -half_pair * cos_psi
    lowered = -hydrogen_reach * cos_phi
    tilted = half_pair * sin_psi * sin_phi
    rest_by = lowered - tilted
    rest_cy = lowered + tilted
    alpha = rest_bx * (oldb_x - oldc_x) + oldb_y * rest_by + oldc_y * rest_cy
    beta = rest_bx * (oldc_y - oldb_y) + oldb_x * rest_by + oldc_x * rest_cy
    gamma = oldb_x * newb_y - newb_x * oldb_y + oldc_x * newc_y - newc_x * oldc_y
    summed = alpha * alpha + beta * beta
    sin_theta = (alpha * gamma - beta * jnp.sqrt(summed - gamma * gamma)) / summed
    cos_theta = jnp.sqrt(1.0 - sin_theta * sin_theta)
    final_ax = -rest_ay * sin_theta
    final_ay = rest_ay * cos_theta
    final_bx = rest_bx * cos_theta - rest_by * sin_theta
    final_by = rest_bx * sin_theta + rest_by * cos_theta
    final_cx = -rest_bx * cos_theta - rest_cy * sin_theta
    final_cy = -rest_bx * sin_theta + rest_cy * cos_theta
    out = []
    for rel, along_x, along_y, along_z in (
        (rel_a, final_ax, final_ay, newa_z),
        (rel_b, final_bx, final_by, newb_z),
        (rel_c, final_cx, final_cy, newc_z),
    ):
        for k in range(3):
            out.append(axis_x[k] * along_x + axis_y[k] * along_y + axis_z[k] * along_z - rel[k])
    return [vel[k] + out[k] / time_step for k in range(9)]


def sort4(x):
    lane = lax.broadcasted_iota(i32, (8, 128), 1)
    sub = lax.broadcasted_iota(i32, (8, 128), 0)
    within = (lane << 5) | (sub << 2)
    x = list(x)
    for k in range(1, 13):
        for j in range(k - 1, -1, -1):
            if j < 2:
                for a in range(4):
                    b = a | (1 << j)
                    if a == b:
                        continue
                    low, high = jnp.minimum(x[a], x[b]), jnp.maximum(x[a], x[b])
                    if k == 12:
                        x[a], x[b] = low, high
                    elif k < 2:
                        x[a], x[b] = (low, high) if not (a >> k) & 1 else (high, low)
                    else:
                        up = ((within >> k) & 1) == 0
                        x[a], x[b] = jnp.where(up, low, high), jnp.where(up, high, low)
                continue
            first = ((within >> j) & 1) == 0
            if k == 12:
                keep_low = first
            else:
                keep_low = ((within >> j) & 1) == ((within >> k) & 1)
            for a in range(4):
                if j < 5:
                    step = 1 << (j - 2)
                    if step == 4:
                        other = pltpu.roll(x[a], 4, 0)
                    else:
                        other = jnp.where(
                            first, pltpu.roll(x[a], 8 - step, 0), pltpu.roll(x[a], step, 0)
                        )
                else:
                    other = take(x[a], lane ^ (1 << (j - 5)))
                x[a] = jnp.where(keep_low, jnp.minimum(x[a], other), jnp.maximum(x[a], other))
    return x


def gather_rows(tables, count, rows, lanes):
    outs = []
    for row_at, lane_at in zip(rows, lanes):
        hits = [row_at == r for r in range(count)]
        got = []
        for table in tables:
            acc = jnp.zeros((8, 128), table(0).dtype)
            for r in range(count):
                acc = jnp.where(hits[r], take(table(r), lane_at), acc)
            got.append(acc)
        outs.append(got)
    return outs


def row_of(ref, *base):
    def read(r):
        return jnp.broadcast_to(ref[base + (pl.ds(r, 1),)] if base else ref[pl.ds(r, 1), :], (8, 128))

    return read


def bonds_as_given(pos, vel, mass, bonds, left, right, block, table, ends, slots):
    for r in range(16):
        at = pl.ds(128 * r, 128)
        for k in range(3):
            table[k, pl.ds(r, 1)] = pos[pl.ds(k, 1), at]
            table[3 + k, pl.ds(r, 1)] = vel[pl.ds(k, 1), at]
        table[6, pl.ds(r, 1)] = mass[pl.ds(r, 1), :]
    for half in range(2):
        ends[pl.ds(16 * half + 8, 8), :] = jnp.full((8, 128), 2048, i32)
        for r in range(10):
            ends[pl.ds(16 * half + r, 1), :] = bonds[pl.ds(half, 1), pl.ds(128 * r, 128)]
    slots[...] = jnp.zeros((8, 128), i32)
    for r in range(3):
        slots[pl.ds(r, 1), :] = right[pl.ds(r, 1), :]
        slots[pl.ds(3 + r, 1), :] = left[pl.ds(r, 1), :]

    tables = [row_of(table, k) for k in range(7)]
    atoms = [ends[pl.ds(8 * q, 8), :] for q in range(4)] + [slots[...]]
    at = gather_rows(tables, 16, [a >> 7 for a in atoms], [a & 127 for a in atoms])
    for q in range(2):
        size = min(8, B - 8 * q)

        def put(base, value):
            block[pl.ds(base + 8 * q, size), :] = value[0:size]

        for k in range(3):
            put(DIFF + B * k, at[q][k] - at[2 + q][k])
            put(DVEL + B * k, at[q][3 + k] - at[2 + q][3 + k])
        put(SCALE, 1.0 / jnp.sqrt(at[q][6] + at[2 + q][6]))
    for k in range(7):
        block[pl.ds(SPOS + S * k, S), :] = at[4][k][0:S]


def order_bonds(ends, before):
    lane = lax.broadcasted_iota(i32, (8, 128), 1)
    sub = lax.broadcasted_iota(i32, (8, 128), 0)
    start = []
    for q in range(4):
        at = sub + 8 * q
        start.append((ends[pl.ds(8 * q, 8), :] << 12) | (at << 7) | lane)
    done = sort4(start)
    for q in range(4):
        before[pl.ds(8 * q, 8), :] = done[q]


def use_order(block, local, table, ends, keys, atoms, before, slots):
    lane = lax.broadcasted_iota(i32, (8, 128), 1)
    sub = lax.broadcasted_iota(i32, (8, 128), 0)
    rows, lanes = [], []
    for q in range(3):
        n = jnp.minimum(lane * E + sub + 8 * q, 4095)
        rows.append(((n & 3) << 3) | ((n >> 2) & 7))
        lanes.append(n >> 5)
    key = [g[0] for g in gather_rows([row_of(before)], 32, rows, lanes)]
    for q in range(3):
        keys[pl.ds(8 * q, 8), :] = key[q]
    atom = [k >> 12 for k in key]
    twin = [(k & 4095) ^ 2048 for k in key]
    other = [
        g[0]
        for g in gather_rows([row_of(ends)], 26, [t >> 7 for t in twin], [t & 127 for t in twin])
    ]

    slot_atom = slots[...]
    own_atom = [(sub + 8 * q) * 128 + lane for q in range(2)]
    queries = [(other[q] << 12) | twin[q] for q in range(3)]
    queries += [(a << 12) | 4095 for a in [slot_atom] + own_atom]
    leaders = jnp.broadcast_to(keys[pl.ds(0, 1), :], (8, 128))
    found_row, found_lane, found_key = [], [], []
    for query in queries:
        low = jnp.zeros((8, 128), i32)
        for bit in (64, 32, 16, 8, 4, 2, 1):
            low = jnp.where(take(leaders, low + bit) <= query, low + bit, low)
        count = jnp.full((8, 128), -1, i32)
        best = jnp.full((8, 128), -1, i32)
        for r in range(E):
            seen = take(jnp.broadcast_to(keys[pl.ds(r, 1), :], (8, 128)), low)
            less = seen <= query
            count = jnp.where(less, count + 1, count)
            best = jnp.where(less, seen, best)
        found_row.append(count)
        found_lane.append(low)
        found_key.append(best)
    places = [found_row[q] * 128 + found_lane[q] for q in range(6)]
    slot_place = jnp.where((found_key[3] >> 12) == slot_atom, places[3], -1)
    for q in range(2):
        place = jnp.where((found_key[4 + q] >> 12) == own_atom[q], places[4 + q], -1)
        local[pl.ds(8 * q, 8), :] = place.astype(f32)

    high = lax.broadcasted_iota(i32, (16, 128), 0)
    code = lax.broadcasted_iota(i32, (16, 128), 1) + 1
    low_of = lax.broadcasted_iota(i32, (128, 128), 0)
    which = jnp.zeros((32, 128), f32)
    for r in range(S):
        here = slots[pl.ds(r, 1), :]
        mine = jnp.broadcast_to(here >> 7, (16, 128)) == high
        left_side = jnp.concatenate(
            [jnp.where(mine, code, 0).astype(f32), jnp.where(mine, r + 1, 0).astype(f32)], axis=0
        )
        right_side = jnp.where(jnp.broadcast_to(here & 127, (128, 128)) == low_of, 1.0, 0.0)
        which = which + lax.dot_general(
            left_side.astype(jnp.bfloat16),
            right_side.astype(jnp.bfloat16),
            (((1,), (1,)), ((), ())),
            preferred_element_type=f32,
        )
    local[pl.ds(16, 16), :] = jnp.where(
        which[0:16] > 0.0, which[16:32] * 128.0 + which[0:16] - 129.0, -1.0
    )

    for q in range(3):
        atoms[pl.ds(8 * q, 8), :] = atom[q]
    before[pl.ds(0, 1), :] = pltpu.roll(atoms[pl.ds(E - 1, 1), :], 1, 1)
    before[pl.ds(1, E - 1), :] = atoms[pl.ds(0, E - 1), :]
    own_rows, own_lanes = [a >> 7 for a in atom], [a & 127 for a in atom]
    own = gather_rows([row_of(table, 6), row_of(local.at[pl.ds(16, 16)])], 16, own_rows, own_lanes)
    for q in range(3):
        size = min(8, E - 8 * q)

        def put(base, value):
            block[pl.ds(base + 8 * q, size), :] = value[0:size]

        put(MASS, own[q][0])
        put(PIDX, places[q].astype(f32))
        same = before[pl.ds(8 * q, 8), :] == atom[q]
        if q == 0:
            same = same & ((lane > 0) | (sub > 0))
        put(CONT, jnp.where(same, 1.0, 0.0))
        put(CIDX, own[q][1])
        put(HIDX, (key[q] & 4095).astype(f32))
    block[pl.ds(SIDX, S), :] = slot_place.astype(f32)[0:S]
    block[pl.ds(SIDX + S, ROWS - SIDX - S), :] = jnp.zeros((ROWS - SIDX - S, 128), f32)


def waters(wpos, wvel, wout, water):
    for k in range(9):
        for r in range(8):
            water[k, pl.ds(r, 1)] = wpos[pl.ds(k, 1), pl.ds(128 * r, 128)]
            water[9 + k, pl.ds(r, 1)] = wvel[pl.ds(k, 1), pl.ds(128 * r, 128)]
    new = settle([water[k] for k in range(9)], [water[9 + k] for k in range(9)])
    for k in range(9):
        water[k] = new[k]
        for r in range(8):
            wout[pl.ds(k, 1), pl.ds(128 * r, 128)] = water[k, pl.ds(r, 1)]


def pick(tables, rows, lanes):
    outs = [[] for _ in tables]
    for row_at, lane_at in zip(rows, lanes):
        hits = [row_at == r for r in range(len(tables[0]))]
        for out, table in zip(outs, tables):
            acc = jnp.zeros((8, 128), f32)
            for hit, part in zip(hits, table):
                acc = jnp.where(hit, take(part, lane_at), acc)
            out.append(acc)
    return outs


def swap(slots):
    back = [pltpu.roll(part, 7, 0) for part in slots[3:6]]
    ahead = [pltpu.roll(part, 1, 0) for part in slots[0:3]]
    return back + ahead


def rounds(
    data, local, vel_in, water, out, water_out,
    w, g, m, prow, plane, crow, clane, cont, pf, pb, x, xt, wc, d, length, scale, delta,
    sw, sm, srow, slane, sww, sx, sxt, sd, slength, sscale, sdelta, wx, vel, vel_sem, water_sem,
):
    load = pltpu.make_async_copy(vel_in, vel, vel_sem)
    load.start()
    passed = pltpu.make_async_copy(water, water_out, water_sem)
    passed.start()

    def rows_at(base, count):
        return [data[:, base + r, :] for r in range(count)]

    for base, row_ref, lane_ref, count in ((PIDX, prow, plane, E), (CIDX, crow, clane, E), (SIDX, srow, slane, S)):
        for r in range(count):
            value = data[:, base + r, :].astype(i32)
            row_ref[r] = value >> 7
            lane_ref[r] = value & 127
    keep = rows_at(CONT, E)
    run = jnp.ones((8, 128), f32)
    for r in range(E):
        cont[r] = keep[r]
        if r > 0:
            run = run * keep[r]
        pf[r] = run
    whole = run
    run = jnp.ones((8, 128), f32)
    for r in range(E - 1, -1, -1):
        pb[r] = run
        run = run * keep[r]
    extra = jnp.max(jnp.sum(whole, axis=1, keepdims=True)).astype(i32)
    opens = keep[0]
    closes = pltpu.roll(opens, 127, 1)

    def geometry(diff, dvel, s):
        far = jnp.sqrt(dot3(diff, diff))
        ratio = s / far
        weight = [ratio * part for part in diff]
        moved = [diff[k] + time_step * dvel[k] for k in range(3)]
        return far, weight, moved, time_step * dot3(weight, dvel)

    own = [rows_at(SPOS + S * k, S) for k in range(7)]
    twin = [swap(part) for part in own]
    for r in range(S):
        diff = [own[k][r] - twin[k][r] for k in range(3)]
        dvel = [own[3 + k][r] - twin[3 + k][r] for k in range(3)]
        s = 1.0 / jnp.sqrt(own[6][r] + twin[6][r])
        far, weight, moved, first = geometry(diff, dvel, s)
        for k in range(3):
            sw[k, r] = weight[k]
            sd[k, r] = moved[k]
            sdelta[k, r] = jnp.zeros((8, 128), f32)
        sm[r] = own[6][r]
        sww[r] = dot3(weight, weight)
        slength[r] = far
        sscale[r] = s
        sx[r] = first
    near = pick(
        [[sw[k, r] for r in range(S)] for k in range(3)],
        [crow[r] for r in range(E)],
        [clane[r] for r in range(E)],
    )
    given = [rows_at(base + B * k, B) for base in (DIFF, DVEL) for k in range(3)]
    half = [data[:, HIDX + r, :].astype(i32) for r in range(E)]
    given = pick(
        given + [rows_at(SCALE, B)], [(h >> 7) & 15 for h in half], [h & 127 for h in half]
    )
    for r in range(E):
        sign = jnp.where(half[r] < 2048, 1.0, -1.0)
        diff = [sign * given[k][r] for k in range(3)]
        dvel = [sign * given[3 + k][r] for k in range(3)]
        s = given[6][r]
        far, weight, moved, first = geometry(diff, dvel, s)
        for k in range(3):
            w[k, r] = weight[k]
            d[k, r] = moved[k]
            wc[k, r] = near[k][r]
            delta[k, r] = jnp.zeros((8, 128), f32)
        g[r] = dot3(weight, [near[k][r] for k in range(3)])
        m[r] = data[:, MASS + r, :]
        length[r] = far
        scale[r] = s
        x[r] = first

    def totals(parts):
        count = len(parts)
        inside = []
        for part in parts:
            acc = part[0]
            fwd = [acc]
            for r in range(1, E):
                acc = part[r] + cont[r] * acc
                fwd.append(acc)
            for r in range(E - 2, -1, -1):
                fwd[r] = jnp.where(cont[r + 1] > 0.0, fwd[r + 1], fwd[r])
            inside.append(fwd)
        ahead = tuple(opens * pltpu.roll(part[E - 1], 1, 1) for part in inside)
        back = tuple(closes * pltpu.roll(part[0], 127, 1) for part in inside)

        def spread(_, now):
            ahead_now, back_now = now[:count], now[count:]
            new = [ahead[k] + opens * pltpu.roll(whole * ahead_now[k], 1, 1) for k in range(count)]
            new += [back[k] + closes * pltpu.roll(whole * back_now[k], 127, 1) for k in range(count)]
            return tuple(new)

        carried = lax.fori_loop(0, extra, spread, ahead + back)
        return [
            [
                inside[k][r] + pf[r] * carried[k] + pb[r] * carried[count + k]
                for r in range(E)
            ]
            for k in range(count)
        ]

    def apply_k(_, carry):
        slot_x = [sx[r] for r in range(S)]
        cross_x = pick([slot_x], [crow[r] for r in range(E)], [clane[r] for r in range(E)])[0]
        sums = totals(
            [[w[k, r] * x[r] for r in range(E)] for k in range(3)]
            + [[g[r] * x[r] for r in range(E)]]
        )
        slot_sum = pick([sums[3]], [srow[r] for r in range(S)], [slane[r] for r in range(S)])[0]
        z = [
            m[r] * (w[0, r] * sums[0][r] + w[1, r] * sums[1][r] + w[2, r] * sums[2][r] + g[r] * cross_x[r])
            for r in range(E)
        ]
        slot_z = [sm[r] * (slot_sum[r] + sww[r] * slot_x[r]) for r in range(S)]
        slot_twin = swap(slot_z)
        for r in range(S):
            new = slot_x[r] - (slot_z[r] + slot_twin[r])
            sx[r] = new
            sxt[r] = sxt[r] + new
        z_twin = pick([z], [prow[r] for r in range(E)], [plane[r] for r in range(E)])[0]
        for r in range(E):
            new = x[r] - (z[r] + z_twin[r])
            x[r] = new
            xt[r] = xt[r] + new
        return carry

    def solve(index, carry):
        for r in range(E):
            xt[r] = x[r]
        for r in range(S):
            sxt[r] = sx[r]
        lax.fori_loop(0, ORDER, apply_k, 0)
        slot_xt = [sxt[r] for r in range(S)]
        cross_x = pick([slot_xt], [crow[r] for r in range(E)], [clane[r] for r in range(E)])[0]
        sums = totals([[w[k, r] * xt[r] for r in range(E)] for k in range(3)])
        for k in range(3):
            for r in range(E):
                delta[k, r] = delta[k, r] - m[r] * (sums[k][r] + wc[k, r] * cross_x[r])
                wx[k, r] = sums[k][r]
            for r in range(S):
                sdelta[k, r] = sdelta[k, r] - sm[r] * (sw[k, r] * slot_xt[r])

        @pl.when(index < ITER)
        def _():
            slot_sum = pick(
                [[wx[k, r] for r in range(E)] for k in range(3)],
                [srow[r] for r in range(S)],
                [slane[r] for r in range(S)],
            )
            for k in range(3):
                for r in range(S):
                    sdelta[k, r] = sdelta[k, r] - sm[r] * slot_sum[k][r]

            def lengthening(gap, far, s):
                target = jnp.sqrt(2.0 * far * far - dot3(gap, gap))
                return s * (far - target)

            here = [[delta[k, r] for r in range(E)] for k in range(3)]
            there = pick(here, [prow[r] for r in range(E)], [plane[r] for r in range(E)])
            for r in range(E):
                gap = [d[k, r] + (here[k][r] - there[k][r]) for k in range(3)]
                x[r] = lengthening(gap, length[r], scale[r])
            here = [[sdelta[k, r] for r in range(S)] for k in range(3)]
            there = [swap(part) for part in here]
            for r in range(S):
                gap = [sd[k, r] + (here[k][r] - there[k][r]) for k in range(3)]
                sx[r] = lengthening(gap, slength[r], sscale[r])

        return carry

    lax.fori_loop(0, ITER + 1, solve, 0)

    me = lax.axis_index("dom")

    def own_row(ref, k):
        return lambda r: jnp.broadcast_to(ref[k, r, pl.ds(me, 1), :], (8, 128))

    load.wait()
    places = [local[pl.ds(8 * q, 8), :].astype(i32) for q in range(4)]
    rows, lanes = [p >> 7 for p in places], [p & 127 for p in places]
    inner = gather_rows([own_row(delta, k) for k in range(3)], E, rows[:2], lanes[:2])
    outer = gather_rows([own_row(sdelta, k) for k in range(3)], S, rows[2:], lanes[2:])
    for q in range(2):
        for k in range(3):
            xt[3 * q + k] = jnp.where(rows[q] >= 0, inner[q][k], outer[q][k])
    for k in range(3):
        for r in range(16):
            at = pl.ds(128 * r, 128)
            change = xt[3 * (r // 8) + k, pl.ds(r % 8, 1), :]
            out[pl.ds(k, 1), at] = vel[pl.ds(k, 1), at] + change / time_step
    passed.wait()


CHUNKS = ((0, 56), (56, 56), (112, 56), (168, 56))


def share(
    pos_in, vel_in, mass_in, bonds_in, left_in, right_in, wpos_in, wvel_in, out, local, wout,
    pos, vel, mass, bonds, left, right, wpos, wvel,
    block, table, ends, keys, atoms, before, slots, water, send, recv, local_sem, load_sem,
):
    me = lax.axis_index("dom")
    count = out.shape[0]
    last = count // 2 - 1
    z, core = me // 2, me % 2
    partner, up, down = 2 * z + 1 - core, me + 2, me - 2

    loads = [
        pltpu.make_async_copy(origin, target, load_sem.at[k])
        for k, (origin, target) in enumerate(
            (
                (bonds_in, bonds), (pos_in, pos), (vel_in, vel), (mass_in, mass),
                (left_in, left), (right_in, right), (wpos_in, wpos), (wvel_in, wvel),
            )
        )
    ]
    for load in loads:
        load.start()
    barrier = pltpu.get_barrier_semaphore()

    def greet(target):
        pl.semaphore_signal(
            barrier, inc=1, device_id={"dom": target}, device_id_type=pl.DeviceIdType.MESH
        )

    greet(partner)

    @pl.when(z < last)
    def _():
        greet(up)

    @pl.when(z > 0)
    def _():
        greet(down)

    @pl.when(z == 0)
    def _():
        greet(me + 2 * last)

    @pl.when(z == last)
    def _():
        greet(me - 2 * last)

    ends_of_line = jnp.where(z == 0, 1, 0) + jnp.where(z == last, 1, 0)
    peers = 1 + jnp.where(z < last, 1, 0) + jnp.where(z > 0, 1, 0) + ends_of_line
    for load in loads[:6]:
        load.wait()
    bonds_as_given(pos, vel, mass, bonds, left, right, block, table, ends, slots)
    pl.semaphore_wait(barrier, peers)

    def copy(origin, source, k, target, sem):
        rows = pl.ds(*CHUNKS[k])
        return pltpu.make_async_remote_copy(
            src_ref=origin.at[rows],
            dst_ref=out.at[source, rows],
            send_sem=send.at[sem, k],
            recv_sem=recv.at[source, k],
            device_id={"dom": target},
            device_id_type=pl.DeviceIdType.MESH,
        )

    sent = []

    def push(when, origin, source, k, target, sem):
        sent.append((when, origin, source, k, target, sem))

        @pl.when(when)
        def _():
            copy(origin, source, k, target, sem).start()

    def give(chunks):
        for k in chunks:
            push(z == 0, block, me, k, me + 2 * last, 15)
            push(z == last, block, me, k, me - 2 * last, 16)
            push(z < last, block, me, k, up, 0)
            push(z > 0, block, me, k, down, 1)
            push(z >= 0, block, me, k, partner, 2)

    def relay(away, chunks):
        for k in chunks:
            for side, arrives, source, onward, target in (
                (0, z >= away, me - 2 * away, z < last, up),
                (1, z + away <= last, me + 2 * away, z > 0, down),
            ):
                sem = 3 + 4 * (away - 1) + 2 * side

                @pl.when(arrives)
                def _(source=source, k=k):
                    copy(out.at[source], source, k, partner, 0).wait_recv()

                if away < last - 1:
                    push(arrives & onward, out.at[source], source, k, target, sem)
                push(arrives, out.at[source], source, k, partner, sem + 1)

    early, late = (0, 1), (2, 3)
    give(early)
    order_bonds(ends, before)
    relay(1, early)
    use_order(block, local, table, ends, keys, atoms, before, slots)
    give(late)
    here = pltpu.make_async_copy(block, out.at[me], local_sem)
    here.start()
    relay(2, early)
    for load in loads[6:]:
        load.wait()
    waters(wpos, wvel, wout, water)
    for away in range(3, last + 1):
        relay(away, early)
    for away in range(1, last + 1):
        relay(away, late)
    for k in range(len(CHUNKS)):
        for chip in range(last + 1):
            source = 2 * chip + 1 - core
            copy(out.at[source], source, k, partner, 0).wait_recv()
    for when, origin, source, k, target, sem in sent:

        @pl.when(when)
        def _(origin=origin, source=source, k=k, target=target, sem=sem):
            copy(origin, source, k, target, sem).wait_send()

    here.wait()


def on_device(
    protein_pos, protein_vel, inv_mass, bond_atoms, left_atoms, right_atoms, water_pos, water_vel
):
    vmem = pl.BlockSpec(memory_space=pltpu.VMEM)
    hbm = pl.BlockSpec(memory_space=pltpu.HBM)
    count = lax.axis_size("dom")
    data, local, water_velocity = pl.pallas_call(
        share,
        out_shape=(
            jax.ShapeDtypeStruct((count, ROWS, 128), f32),
            jax.ShapeDtypeStruct((32, 128), f32),
            jax.ShapeDtypeStruct(water_pos.shape, f32),
        ),
        in_specs=[hbm] * 8,
        out_specs=(vmem,) * 3,
        scratch_shapes=[
            pltpu.VMEM(protein_pos.shape, f32),
            pltpu.VMEM(protein_vel.shape, f32),
            pltpu.VMEM((16, 128), f32),
            pltpu.VMEM(bond_atoms.shape, i32),
            pltpu.VMEM((3, 128), i32),
            pltpu.VMEM((3, 128), i32),
            pltpu.VMEM(water_pos.shape, f32),
            pltpu.VMEM(water_vel.shape, f32),
            pltpu.VMEM((ROWS, 128), f32),
            pltpu.VMEM((7, 16, 128), f32),
            pltpu.VMEM((32, 128), i32),
            pltpu.VMEM((24, 128), i32),
            pltpu.VMEM((24, 128), i32),
            pltpu.VMEM((32, 128), i32),
            pltpu.VMEM((8, 128), i32),
            pltpu.VMEM((18, 8, 128), f32),
            pltpu.SemaphoreType.DMA((17, len(CHUNKS))),
            pltpu.SemaphoreType.DMA((count, len(CHUNKS))),
            pltpu.SemaphoreType.DMA,
            pltpu.SemaphoreType.DMA((8,)),
        ],
        compiler_params=pltpu.CompilerParams(
            collective_id=0, has_side_effects=True, vmem_limit_bytes=16 * 2**20
        ),
        name="share",
    )(
        *(
            pltpu.with_memory_space_constraint(value, pltpu.HBM)
            for value in (
                protein_pos,
                protein_vel,
                inv_mass.reshape(16, 128),
                bond_atoms,
                left_atoms.reshape(3, 128),
                right_atoms.reshape(3, 128),
                water_pos,
                water_vel,
            )
        )
    )
    scratch = [
        ((3, E), f32), ((E,), f32), ((E,), f32),
        ((E,), i32), ((E,), i32), ((E,), i32), ((E,), i32),
        ((E,), f32), ((E,), f32), ((E,), f32),
        ((E,), f32), ((E,), f32),
        ((3, E), f32), ((3, E), f32), ((E,), f32), ((E,), f32), ((3, E), f32),
        ((3, S), f32), ((S,), f32), ((S,), i32), ((S,), i32), ((S,), f32),
        ((S,), f32), ((S,), f32), ((3, S), f32), ((S,), f32), ((S,), f32), ((3, S), f32),
        ((3, E), f32),
    ]
    protein_velocity, water_velocity = pl.pallas_call(
        rounds,
        out_shape=(
            jax.ShapeDtypeStruct(protein_vel.shape, f32),
            jax.ShapeDtypeStruct(water_vel.shape, f32),
        ),
        in_specs=[vmem, vmem, hbm, vmem],
        out_specs=(vmem, hbm),
        scratch_shapes=[pltpu.VMEM(shape + (8, 128), kind) for shape, kind in scratch]
        + [pltpu.VMEM(protein_vel.shape, f32), pltpu.SemaphoreType.DMA, pltpu.SemaphoreType.DMA],
        compiler_params=pltpu.CompilerParams(vmem_limit_bytes=16 * 2**20),
        name="rounds",
    )(data, local, pltpu.with_memory_space_constraint(protein_vel, pltpu.HBM), water_velocity)
    return (protein_velocity, water_velocity)


def solution(mesh):
    in_specs = (
        P(None, ("rep", "dom")),
        P(None, ("rep", "dom")),
        P(("rep", "dom")),
        P(None, ("rep", "dom")),
        P(("rep", "dom")),
        P(("rep", "dom")),
        P(None, ("rep", "dom")),
        P(None, ("rep", "dom")),
    )
    out_specs = (P(None, ("rep", "dom")), P(None, ("rep", "dom")))
    return jax.shard_map(
        on_device, mesh=mesh, in_specs=in_specs, out_specs=out_specs, check_vma=False
    )
```

```python
import functools
import math

import jax
import jax.numpy as jnp
from jax import lax
from jax.experimental import pallas as pl
from jax.experimental.pallas import tpu as pltpu
from jax.sharding import PartitionSpec as P

ORDER = 4
ITER = 2

time_step = 0.002
mass_oxygen = 15.9994
mass_hydrogen = 1.008
oxygen_hydrogen = 0.09572
hydrogen_pair = 0.15139
total_mass = mass_oxygen + 2.0 * mass_hydrogen
half_pair = 0.5 * hydrogen_pair
water_height = math.sqrt(oxygen_hydrogen * oxygen_hydrogen - half_pair * half_pair)
oxygen_reach = 2.0 * mass_hydrogen * water_height / total_mass
hydrogen_reach = water_height - oxygen_reach

B = 10
S = 6
DIFF, DVEL, SCALE, SPOS = 0, 3 * B, 6 * B, 7 * B
SVEL, SMASS = SPOS + 3 * S, SPOS + 6 * S
EARLY = SPOS + 7 * S
E = 20
PANEL = 7
MASS, PIDX, CONT, CIDX, HIDX = EARLY, EARLY + E, EARLY + 2 * E, EARLY + 3 * E, EARLY + 4 * E
SIDX = EARLY + 5 * E
ROWS = 224
f32, i32 = jnp.float32, jnp.int32


def take(table, lanes):
    return jnp.take_along_axis(table, lanes, axis=1, mode="promise_in_bounds")


def cross3(a, b):
    return (
        a[1] * b[2] - a[2] * b[1],
        a[2] * b[0] - a[0] * b[2],
        a[0] * b[1] - a[1] * b[0],
    )


def dot3(a, b):
    return a[0] * b[0] + a[1] * b[1] + a[2] * b[2]


def settle(old, vel):
    old_b = [old[3 + k] - old[k] for k in range(3)]
    old_c = [old[6 + k] - old[k] for k in range(3)]
    new_a = [time_step * vel[k] for k in range(3)]
    new_b = [old_b[k] + time_step * vel[3 + k] for k in range(3)]
    new_c = [old_c[k] + time_step * vel[6 + k] for k in range(3)]
    center = [
        (mass_oxygen * new_a[k] + mass_hydrogen * (new_b[k] + new_c[k])) / total_mass
        for k in range(3)
    ]
    rel_a = [new_a[k] - center[k] for k in range(3)]
    rel_b = [new_b[k] - center[k] for k in range(3)]
    rel_c = [new_c[k] - center[k] for k in range(3)]
    normal = cross3(old_b, old_c)
    side = cross3(rel_a, normal)
    upward = cross3(normal, side)

    def norm(vec):
        size = jnp.sqrt(dot3(vec, vec))
        return [part / size for part in vec]

    axis_z, axis_x, axis_y = norm(normal), norm(side), norm(upward)
    oldb_x, oldb_y = dot3(axis_x, old_b), dot3(axis_y, old_b)
    oldc_x, oldc_y = dot3(axis_x, old_c), dot3(axis_y, old_c)
    newa_z = dot3(axis_z, rel_a)
    newb_x, newb_y, newb_z = dot3(axis_x, rel_b), dot3(axis_y, rel_b), dot3(axis_z, rel_b)
    newc_x, newc_y, newc_z = dot3(axis_x, rel_c), dot3(axis_y, rel_c), dot3(axis_z, rel_c)
    sin_phi = newa_z / oxygen_reach
    cos_phi = jnp.sqrt(1.0 - sin_phi * sin_phi)
    sin_psi = (newb_z - newc_z) / (2.0 * half_pair * cos_phi)
    cos_psi = jnp.sqrt(1.0 - sin_psi * sin_psi)
    rest_ay = oxygen_reach * cos_phi
    rest_bx = -half_pair * cos_psi
    lowered = -hydrogen_reach * cos_phi
    tilted = half_pair * sin_psi * sin_phi
    rest_by = lowered - tilted
    rest_cy = lowered + tilted
    alpha = rest_bx * (oldb_x - oldc_x) + oldb_y * rest_by + oldc_y * rest_cy
    beta = rest_bx * (oldc_y - oldb_y) + oldb_x * rest_by + oldc_x * rest_cy
    gamma = oldb_x * newb_y - newb_x * oldb_y + oldc_x * newc_y - newc_x * oldc_y
    summed = alpha * alpha + beta * beta
    sin_theta = (alpha * gamma - beta * jnp.sqrt(summed - gamma * gamma)) / summed
    cos_theta = jnp.sqrt(1.0 - sin_theta * sin_theta)
    final_ax = -rest_ay * sin_theta
    final_ay = rest_ay * cos_theta
    final_bx = rest_bx * cos_theta - rest_by * sin_theta
    final_by = rest_bx * sin_theta + rest_by * cos_theta
    final_cx = -rest_bx * cos_theta - rest_cy * sin_theta
    final_cy = -rest_bx * sin_theta + rest_cy * cos_theta
    out = []
    for rel, along_x, along_y, along_z in (
        (rel_a, final_ax, final_ay, newa_z),
        (rel_b, final_bx, final_by, newb_z),
        (rel_c, final_cx, final_cy, newc_z),
    ):
        for k in range(3):
            out.append(axis_x[k] * along_x + axis_y[k] * along_y + axis_z[k] * along_z - rel[k])
    return [vel[k] + out[k] / time_step for k in range(9)]


def sort4(x):
    lane = lax.broadcasted_iota(i32, (8, 128), 1)
    sub = lax.broadcasted_iota(i32, (8, 128), 0)
    within = (lane << 5) | (sub << 2)
    x = list(x)
    for k in range(1, 13):
        for j in range(k - 1, -1, -1):
            if j < 2:
                for a in range(4):
                    b = a | (1 << j)
                    if a == b:
                        continue
                    low, high = jnp.minimum(x[a], x[b]), jnp.maximum(x[a], x[b])
                    if k == 12:
                        x[a], x[b] = low, high
                    elif k < 2:
                        x[a], x[b] = (low, high) if not (a >> k) & 1 else (high, low)
                    else:
                        up = ((within >> k) & 1) == 0
                        x[a], x[b] = jnp.where(up, low, high), jnp.where(up, high, low)
                continue
            first = ((within >> j) & 1) == 0
            if k == 12:
                keep_low = first
            else:
                keep_low = ((within >> j) & 1) == ((within >> k) & 1)
            for a in range(4):
                if j < 5:
                    step = 1 << (j - 2)
                    if step == 4:
                        other = pltpu.roll(x[a], 4, 0)
                    else:
                        other = jnp.where(
                            first, pltpu.roll(x[a], 8 - step, 0), pltpu.roll(x[a], step, 0)
                        )
                else:
                    other = take(x[a], lane ^ (1 << (j - 5)))
                x[a] = jnp.where(keep_low, jnp.minimum(x[a], other), jnp.maximum(x[a], other))
    return x


def gather_rows(tables, count, rows, lanes):
    outs = []
    for row_at, lane_at in zip(rows, lanes):
        hits = [row_at == r for r in range(count)]
        got = []
        for table in tables:
            acc = jnp.zeros((8, 128), table(0).dtype)
            for r in range(count):
                acc = jnp.where(hits[r], take(table(r), lane_at), acc)
            got.append(acc)
        outs.append(got)
    return outs


def row_of(ref, *base):
    def read(r):
        return jnp.broadcast_to(ref[base + (pl.ds(r, 1),)] if base else ref[pl.ds(r, 1), :], (8, 128))

    return read


def bonds_as_given(pos, vel, mass, bonds, left, right, block, table, ends, slots):
    for r in range(16):
        at = pl.ds(128 * r, 128)
        for k in range(3):
            table[k, pl.ds(r, 1)] = pos[pl.ds(k, 1), at]
            table[3 + k, pl.ds(r, 1)] = vel[pl.ds(k, 1), at]
        table[6, pl.ds(r, 1)] = mass[pl.ds(r, 1), :]
    for half in range(2):
        ends[pl.ds(16 * half + 8, 8), :] = jnp.full((8, 128), 2048, i32)
        for r in range(10):
            ends[pl.ds(16 * half + r, 1), :] = bonds[pl.ds(half, 1), pl.ds(128 * r, 128)]
    slots[...] = jnp.zeros((8, 128), i32)
    for r in range(3):
        slots[pl.ds(r, 1), :] = right[pl.ds(r, 1), :]
        slots[pl.ds(3 + r, 1), :] = left[pl.ds(r, 1), :]

    tables = [row_of(table, k) for k in range(7)]
    atoms = [ends[pl.ds(8 * q, 8), :] for q in range(4)] + [slots[...]]
    at = gather_rows(tables, 16, [a >> 7 for a in atoms], [a & 127 for a in atoms])
    for q in range(2):
        size = min(8, B - 8 * q)

        def put(base, value):
            block[pl.ds(base + 8 * q, size), :] = value[0:size]

        for k in range(3):
            put(DIFF + B * k, at[q][k] - at[2 + q][k])
            put(DVEL + B * k, at[q][3 + k] - at[2 + q][3 + k])
        put(SCALE, 1.0 / jnp.sqrt(at[q][6] + at[2 + q][6]))
    for k in range(7):
        block[pl.ds(SPOS + S * k, S), :] = at[4][k][0:S]


def order_bonds(ends, before, local, slots):
    lane = lax.broadcasted_iota(i32, (8, 128), 1)
    sub = lax.broadcasted_iota(i32, (8, 128), 0)
    high = lax.broadcasted_iota(i32, (16, 128), 0)
    code = lax.broadcasted_iota(i32, (16, 128), 1) + 1
    low_of = lax.broadcasted_iota(i32, (128, 128), 0)
    which = jnp.zeros((32, 128), f32)
    for r in range(S):
        here = slots[pl.ds(r, 1), :]
        mine = jnp.broadcast_to(here >> 7, (16, 128)) == high
        left_side = jnp.concatenate(
            [jnp.where(mine, code, 0).astype(f32), jnp.where(mine, r + 1, 0).astype(f32)], axis=0
        )
        right_side = jnp.where(jnp.broadcast_to(here & 127, (128, 128)) == low_of, 1.0, 0.0)
        which = which + lax.dot_general(
            left_side.astype(jnp.bfloat16),
            right_side.astype(jnp.bfloat16),
            (((1,), (1,)), ((), ())),
            preferred_element_type=f32,
        )
    local[pl.ds(16, 16), :] = jnp.where(
        which[0:16] > 0.0, which[16:32] * 128.0 + which[0:16] - 129.0, -1.0
    )
    atom = [ends[pl.ds(8 * q, 8), :] for q in range(4)]
    slot = gather_rows(
        [row_of(local.at[pl.ds(16, 16)])], 16, [a >> 7 for a in atom], [a & 127 for a in atom]
    )
    start = []
    for q in range(4):
        inner = jnp.where((slot[q][0] >= 0.0) & (atom[q] < 2048), 0, 1 << 24)
        start.append(inner | (atom[q] << 12) | ((sub + 8 * q) << 7) | lane)
    done = sort4(start)
    for q in range(4):
        before[pl.ds(8 * q, 8), :] = done[q]


def use_order(block, local, table, ends, keys, atoms, before, slots):
    lane = lax.broadcasted_iota(i32, (8, 128), 1)
    sub = lax.broadcasted_iota(i32, (8, 128), 0)
    rows, lanes = [], []
    for q in range(3):
        row = sub + 8 * q
        n = jnp.where(
            row < PANEL,
            lane * PANEL + row,
            jnp.minimum(lane * (E - PANEL) + row + PANEL * 127, 4095),
        )
        rows.append(((n & 3) << 3) | ((n >> 2) & 7))
        lanes.append(n >> 5)
    key = [g[0] for g in gather_rows([row_of(before)], 32, rows, lanes)]
    for q in range(3):
        keys[pl.ds(8 * q, 8), :] = key[q]
    atom = [(k >> 12) & 4095 for k in key]
    twin = [(k & 4095) ^ 2048 for k in key]
    other = [
        g[0]
        for g in gather_rows([row_of(ends)], 26, [t >> 7 for t in twin], [t & 127 for t in twin])
    ]

    slot_atom = slots[...]
    own_atom = [(sub + 8 * q) * 128 + lane for q in range(2)]
    slots_of = row_of(local.at[pl.ds(16, 16)])
    far_slot = gather_rows([slots_of], 16, [a >> 7 for a in other], [a & 127 for a in other])
    far_inner = [jnp.where(g[0] >= 0.0, 0, 1 << 24) for g in far_slot]
    own_inner = [jnp.where(local[pl.ds(16 + 8 * q, 8), :] >= 0.0, 0, 1 << 24) for q in range(2)]
    queries = [far_inner[q] | (other[q] << 12) | twin[q] for q in range(3)]
    queries += [(slot_atom << 12) | 4095]
    queries += [own_inner[q] | (own_atom[q] << 12) | 4095 for q in range(2)]
    leaders = [jnp.broadcast_to(keys[pl.ds(r, 1), :], (8, 128)) for r in (0, PANEL)]
    border = take(leaders[1], jnp.zeros((8, 128), i32))
    found_row, found_lane, found_key = [], [], []
    for query in queries:
        low = jnp.zeros((8, 128), i32)
        second = query >= border
        for bit in (64, 32, 16, 8, 4, 2, 1):
            leader = jnp.where(second, take(leaders[1], low + bit), take(leaders[0], low + bit))
            low = jnp.where(leader <= query, low + bit, low)
        count = jnp.where(second, PANEL - 1, -1)
        best = jnp.full((8, 128), -1, i32)
        for r in range(E):
            seen = take(jnp.broadcast_to(keys[pl.ds(r, 1), :], (8, 128)), low)
            less = (seen <= query) & (second if r >= PANEL else ~second)
            count = jnp.where(less, count + 1, count)
            best = jnp.where(less, seen, best)
        found_row.append(count)
        found_lane.append(low)
        found_key.append(best)
    places = [found_row[q] * 128 + found_lane[q] for q in range(6)]
    slot_place = jnp.where((found_key[3] >> 12) == slot_atom, places[3], -1)
    for q in range(2):
        place = jnp.where(((found_key[4 + q] >> 12) & 4095) == own_atom[q], places[4 + q], -1)
        local[pl.ds(8 * q, 8), :] = place.astype(f32)

    for q in range(3):
        atoms[pl.ds(8 * q, 8), :] = atom[q]
    before[pl.ds(1, E - 1), :] = atoms[pl.ds(0, E - 1), :]
    first_ends = pltpu.roll(atoms[pl.ds(PANEL - 1, 1), :], 1, 1)
    second_ends = pltpu.roll(atoms[pl.ds(E - 1, 1), :], 1, 1)
    before[pl.ds(0, 1), :] = first_ends
    before[pl.ds(PANEL, 1), :] = jnp.where(
        lax.broadcasted_iota(i32, (1, 128), 1) == 0, first_ends, second_ends
    )
    own_rows, own_lanes = [a >> 7 for a in atom], [a & 127 for a in atom]
    own = gather_rows([row_of(table, 6), row_of(local.at[pl.ds(16, 16)])], 16, own_rows, own_lanes)
    for q in range(3):
        size = min(8, E - 8 * q)

        def put(base, value):
            block[pl.ds(base + 8 * q, size), :] = value[0:size]

        put(MASS, own[q][0])
        put(PIDX, places[q].astype(f32))
        same = before[pl.ds(8 * q, 8), :] == atom[q]
        if q == 0:
            same = same & ((lane > 0) | (sub > 0))
        put(CONT, jnp.where(same, 1.0, 0.0))
        put(CIDX, own[q][1])
        put(HIDX, (key[q] & 4095).astype(f32))
    block[pl.ds(SIDX, S), :] = slot_place.astype(f32)[0:S]
    block[pl.ds(SIDX + S, ROWS - SIDX - S), :] = jnp.zeros((ROWS - SIDX - S, 128), f32)


def waters(wpos, wvel, wout, water):
    for k in range(9):
        for r in range(8):
            water[k, pl.ds(r, 1)] = wpos[pl.ds(k, 1), pl.ds(128 * r, 128)]
            water[9 + k, pl.ds(r, 1)] = wvel[pl.ds(k, 1), pl.ds(128 * r, 128)]
    new = settle([water[k] for k in range(9)], [water[9 + k] for k in range(9)])
    for k in range(9):
        water[k] = new[k]
        for r in range(8):
            wout[pl.ds(k, 1), pl.ds(128 * r, 128)] = water[k, pl.ds(r, 1)]


def pick(tables, rows, lanes):
    outs = [[] for _ in tables]
    for row_at, lane_at in zip(rows, lanes):
        hits = [row_at == r for r in range(len(tables[0]))]
        for out, table in zip(outs, tables):
            acc = jnp.zeros((8, 128), f32)
            for hit, part in zip(hits, table):
                acc = jnp.where(hit, take(part, lane_at), acc)
            out.append(acc)
    return outs


def swap(slots):
    back = [pltpu.roll(part, 7, 0) for part in slots[3:6]]
    ahead = [pltpu.roll(part, 1, 0) for part in slots[0:3]]
    return back + ahead


def rounds(
    data, local, vel_in, water, out, water_out,
    w, g, m, prow, plane, crow, clane, cont, pf, pb, x, xt, wc, d, length, scale, delta,
    sw, sm, srow, slane, sww, sx, sxt, sd, slength, sscale, sdelta, wx, cx, sz, vel, vel_sem, water_sem,
):
    load = pltpu.make_async_copy(vel_in, vel, vel_sem)
    load.start()
    passed = pltpu.make_async_copy(water, water_out, water_sem)
    passed.start()

    def rows_at(base, count):
        return [data[:, base + r, :] for r in range(count)]

    for base, row_ref, lane_ref, count in ((PIDX, prow, plane, E), (CIDX, crow, clane, E), (SIDX, srow, slane, S)):
        for r in range(count):
            value = data[:, base + r, :].astype(i32)
            row_ref[r] = value >> 7
            lane_ref[r] = value & 127
    keep = rows_at(CONT, E)
    for r in range(E):
        cont[r] = keep[r]
    first_lane = lax.broadcasted_iota(i32, (8, 128), 1) == 0
    last_lane = lax.broadcasted_iota(i32, (8, 128), 1) == 127
    panels = (range(PANEL), range(PANEL, E))
    whole = []
    for panel in panels:
        run = jnp.ones((8, 128), f32)
        for r in panel:
            if r > panel[0]:
                run = run * keep[r]
            pf[r] = run
        whole.append(run)
        run = jnp.ones((8, 128), f32)
        for r in reversed(panel):
            pb[r] = run
            run = run * keep[r]
    extra = jnp.max(jnp.sum(whole[0] + whole[1], axis=1, keepdims=True)).astype(i32)

    def from_left(ends):
        one, two = (pltpu.roll(part, 1, 1) for part in ends)
        return [keep[0] * one, keep[PANEL] * jnp.where(first_lane, one, two)]

    def from_right(starts):
        one, two = (pltpu.roll(keep[panel[0]] * part, 127, 1) for panel, part in zip(panels, starts))
        return [jnp.where(last_lane, two, one), jnp.where(last_lane, 0.0, two)]

    spilt = data[:, CIDX + PANEL, :]
    for r in range(PANEL + 1, E):
        spilt = jnp.maximum(spilt, data[:, CIDX + r, :])
    spilt = jnp.max(spilt) >= 0.0

    def geometry(diff, dvel, s):
        far = jnp.sqrt(dot3(diff, diff))
        ratio = s / far
        weight = [ratio * part for part in diff]
        moved = [diff[k] + time_step * dvel[k] for k in range(3)]
        return far, weight, moved, time_step * dot3(weight, dvel)

    own = [rows_at(SPOS + S * k, S) for k in range(7)]
    twin = [swap(part) for part in own]
    for r in range(S):
        diff = [own[k][r] - twin[k][r] for k in range(3)]
        dvel = [own[3 + k][r] - twin[3 + k][r] for k in range(3)]
        s = 1.0 / jnp.sqrt(own[6][r] + twin[6][r])
        far, weight, moved, first = geometry(diff, dvel, s)
        for k in range(3):
            sw[k, r] = weight[k]
            sd[k, r] = moved[k]
            sdelta[k, r] = jnp.zeros((8, 128), f32)
        sm[r] = own[6][r]
        sww[r] = dot3(weight, weight)
        slength[r] = far
        sscale[r] = s
        sx[r] = first
    def to_entries(tables, refs):
        for some, when in ((range(PANEL), None), (range(PANEL, E), spilt)):

            def fill(some=some):
                got = pick(
                    [[part() for part in table] for table in tables],
                    [crow[r] for r in some],
                    [clane[r] for r in some],
                )
                for ref, part in zip(refs, got):
                    for r, value in zip(some, part):
                        ref[r] = value

            if when is None:
                fill()
            else:
                pl.when(when)(fill)

    for r in range(PANEL, E):
        cx[r] = jnp.zeros((8, 128), f32)
        for k in range(3):
            wc[k, r] = jnp.zeros((8, 128), f32)
    to_entries(
        [[functools.partial(lambda k, r: sw[k, r], k, r) for r in range(S)] for k in range(3)],
        [wc.at[k] for k in range(3)],
    )
    given = [rows_at(base + B * k, B) for base in (DIFF, DVEL) for k in range(3)]
    half = [data[:, HIDX + r, :].astype(i32) for r in range(E)]
    given = pick(
        given + [rows_at(SCALE, B)], [(h >> 7) & 15 for h in half], [h & 127 for h in half]
    )
    for r in range(E):
        sign = jnp.where(half[r] < 2048, 1.0, -1.0)
        diff = [sign * given[k][r] for k in range(3)]
        dvel = [sign * given[3 + k][r] for k in range(3)]
        s = given[6][r]
        far, weight, moved, first = geometry(diff, dvel, s)
        for k in range(3):
            w[k, r] = weight[k]
            d[k, r] = moved[k]
            delta[k, r] = jnp.zeros((8, 128), f32)
        g[r] = dot3(weight, [wc[k, r] for k in range(3)])
        m[r] = data[:, MASS + r, :]
        length[r] = far
        scale[r] = s
        x[r] = first

    def totals(parts):
        inside = []
        for part in parts:
            fwd = list(part)
            for panel in panels:
                for r in panel[1:]:
                    fwd[r] = part[r] + cont[r] * fwd[r - 1]
                for r in reversed(panel[:-1]):
                    fwd[r] = jnp.where(cont[r + 1] > 0.0, fwd[r + 1], fwd[r])
            inside.append(fwd)
        start = []
        for part in inside:
            start += from_left([part[PANEL - 1], part[E - 1]])
            start += from_right([part[0], part[PANEL]])

        def spread(_, now):
            new = []
            for k in range(0, len(start), 4):
                left = from_left([whole[0] * now[k], whole[1] * now[k + 1]])
                right = from_right([whole[0] * now[k + 2], whole[1] * now[k + 3]])
                new += [a + b for a, b in zip(start[k : k + 4], left + right)]
            return tuple(new)

        carried = lax.fori_loop(0, extra, spread, tuple(start))
        out = []
        for k, part in enumerate(inside):
            left, right = carried[4 * k : 4 * k + 2], carried[4 * k + 2 : 4 * k + 4]
            out.append(
                [
                    part[r] + pf[r] * left[r >= PANEL] + pb[r] * right[r >= PANEL]
                    for r in range(E)
                ]
            )
        return out

    def to_slots(parts, refs):
        rows, lanes = [srow[r] for r in range(S)], [slane[r] for r in range(S)]
        got = pick([part[:PANEL] for part in parts], rows, lanes)
        for ref, part in zip(refs, got):
            for r in range(S):
                ref[r] = part[r]

        @pl.when(spilt)
        def _():
            rest = pick([part[PANEL:] for part in parts], [row - PANEL for row in rows], lanes)
            for ref, part in zip(refs, rest):
                for r in range(S):
                    ref[r] = ref[r] + part[r]

    def apply_k(_, carry):
        slot_x = [sx[r] for r in range(S)]
        to_entries([[functools.partial(lambda r: sx[r], r) for r in range(S)]], [cx])
        sums = totals(
            [[w[k, r] * x[r] for r in range(E)] for k in range(3)]
            + [[g[r] * x[r] for r in range(E)]]
        )
        to_slots([sums[3]], [sz.at[0]])
        z = [
            m[r] * (w[0, r] * sums[0][r] + w[1, r] * sums[1][r] + w[2, r] * sums[2][r] + g[r] * cx[r])
            for r in range(E)
        ]
        slot_z = [sm[r] * (sz[0, r] + sww[r] * slot_x[r]) for r in range(S)]
        slot_twin = swap(slot_z)
        for r in range(S):
            new = slot_x[r] - (slot_z[r] + slot_twin[r])
            sx[r] = new
            sxt[r] = sxt[r] + new
        z_twin = pick([z], [prow[r] for r in range(E)], [plane[r] for r in range(E)])[0]
        for r in range(E):
            new = x[r] - (z[r] + z_twin[r])
            x[r] = new
            xt[r] = xt[r] + new
        return carry

    def solve(index, carry):
        for r in range(E):
            xt[r] = x[r]
        for r in range(S):
            sxt[r] = sx[r]
        lax.fori_loop(0, ORDER, apply_k, 0)
        slot_xt = [sxt[r] for r in range(S)]
        to_entries([[functools.partial(lambda r: sxt[r], r) for r in range(S)]], [cx])
        sums = totals([[w[k, r] * xt[r] for r in range(E)] for k in range(3)])
        for k in range(3):
            for r in range(E):
                delta[k, r] = delta[k, r] - m[r] * (sums[k][r] + wc[k, r] * cx[r])
                wx[k, r] = sums[k][r]
            for r in range(S):
                sdelta[k, r] = sdelta[k, r] - sm[r] * (sw[k, r] * slot_xt[r])

        @pl.when(index < ITER)
        def _():
            to_slots([[wx[k, r] for r in range(E)] for k in range(3)], [sz.at[k] for k in range(3)])
            for k in range(3):
                for r in range(S):
                    sdelta[k, r] = sdelta[k, r] - sm[r] * sz[k, r]

            def lengthening(gap, far, s):
                target = jnp.sqrt(2.0 * far * far - dot3(gap, gap))
                return s * (far - target)

            here = [[delta[k, r] for r in range(E)] for k in range(3)]
            there = pick(here, [prow[r] for r in range(E)], [plane[r] for r in range(E)])
            for r in range(E):
                gap = [d[k, r] + (here[k][r] - there[k][r]) for k in range(3)]
                x[r] = lengthening(gap, length[r], scale[r])
            here = [[sdelta[k, r] for r in range(S)] for k in range(3)]
            there = [swap(part) for part in here]
            for r in range(S):
                gap = [sd[k, r] + (here[k][r] - there[k][r]) for k in range(3)]
                sx[r] = lengthening(gap, slength[r], sscale[r])

        return carry

    lax.fori_loop(0, ITER + 1, solve, 0)

    me = lax.axis_index("dom")

    def own_row(ref, k):
        return lambda r: jnp.broadcast_to(ref[k, r, pl.ds(me, 1), :], (8, 128))

    load.wait()
    places = [local[pl.ds(8 * q, 8), :].astype(i32) for q in range(4)]
    rows, lanes = [p >> 7 for p in places], [p & 127 for p in places]
    inner = gather_rows([own_row(delta, k) for k in range(3)], E, rows[:2], lanes[:2])
    outer = gather_rows([own_row(sdelta, k) for k in range(3)], S, rows[2:], lanes[2:])
    for q in range(2):
        for k in range(3):
            xt[3 * q + k] = jnp.where(rows[q] >= 0, inner[q][k], outer[q][k])
    for k in range(3):
        for r in range(16):
            at = pl.ds(128 * r, 128)
            change = xt[3 * (r // 8) + k, pl.ds(r % 8, 1), :]
            out[pl.ds(k, 1), at] = vel[pl.ds(k, 1), at] + change / time_step
    passed.wait()


CHUNKS = ((0, 56), (56, 56), (112, 56), (168, 56))


def share(
    pos_in, vel_in, mass_in, bonds_in, left_in, right_in, wpos_in, wvel_in, out, local, wout,
    pos, vel, mass, bonds, left, right, wpos, wvel,
    block, table, ends, keys, atoms, before, slots, water, send, recv, local_sem, load_sem,
):
    me = lax.axis_index("dom")
    count = out.shape[0]
    last = count // 2 - 1
    z, core = me // 2, me % 2
    partner, up, down = 2 * z + 1 - core, me + 2, me - 2

    loads = [
        pltpu.make_async_copy(origin, target, load_sem.at[k])
        for k, (origin, target) in enumerate(
            (
                (bonds_in, bonds), (pos_in, pos), (vel_in, vel), (mass_in, mass),
                (left_in, left), (right_in, right), (wpos_in, wpos), (wvel_in, wvel),
            )
        )
    ]
    for load in loads:
        load.start()
    barrier = pltpu.get_barrier_semaphore()

    def greet(target):
        pl.semaphore_signal(
            barrier, inc=1, device_id={"dom": target}, device_id_type=pl.DeviceIdType.MESH
        )

    greet(partner)

    @pl.when(z < last)
    def _():
        greet(up)

    @pl.when(z > 0)
    def _():
        greet(down)

    @pl.when(z == 0)
    def _():
        greet(me + 2 * last)

    @pl.when(z == last)
    def _():
        greet(me - 2 * last)

    ends_of_line = jnp.where(z == 0, 1, 0) + jnp.where(z == last, 1, 0)
    peers = 1 + jnp.where(z < last, 1, 0) + jnp.where(z > 0, 1, 0) + ends_of_line
    for load in loads[:6]:
        load.wait()
    bonds_as_given(pos, vel, mass, bonds, left, right, block, table, ends, slots)
    pl.semaphore_wait(barrier, peers)

    def copy(origin, source, k, target, sem):
        rows = pl.ds(*CHUNKS[k])
        return pltpu.make_async_remote_copy(
            src_ref=origin.at[rows],
            dst_ref=out.at[source, rows],
            send_sem=send.at[sem, k],
            recv_sem=recv.at[source, k],
            device_id={"dom": target},
            device_id_type=pl.DeviceIdType.MESH,
        )

    sent = []

    def push(when, origin, source, k, target, sem):
        sent.append((when, origin, source, k, target, sem))

        @pl.when(when)
        def _():
            copy(origin, source, k, target, sem).start()

    def give(chunks):
        for k in chunks:
            push(z == 0, block, me, k, me + 2 * last, 15)
            push(z == last, block, me, k, me - 2 * last, 16)
            push(z < last, block, me, k, up, 0)
            push(z > 0, block, me, k, down, 1)
            push(z >= 0, block, me, k, partner, 2)

    def relay(away, chunks):
        for k in chunks:
            for side, arrives, source, onward, target in (
                (0, z >= away, me - 2 * away, z < last, up),
                (1, z + away <= last, me + 2 * away, z > 0, down),
            ):
                sem = 3 + 4 * (away - 1) + 2 * side

                @pl.when(arrives)
                def _(source=source, k=k):
                    copy(out.at[source], source, k, partner, 0).wait_recv()

                if away < last - 1:
                    push(arrives & onward, out.at[source], source, k, target, sem)
                push(arrives, out.at[source], source, k, partner, sem + 1)

    early, late = (0, 1), (2, 3)
    give(early)
    order_bonds(ends, before, local, slots)
    relay(1, early)
    use_order(block, local, table, ends, keys, atoms, before, slots)
    give(late)
    here = pltpu.make_async_copy(block, out.at[me], local_sem)
    here.start()
    relay(2, early)
    for load in loads[6:]:
        load.wait()
    waters(wpos, wvel, wout, water)
    for away in range(3, last + 1):
        relay(away, early)
    for away in range(1, last + 1):
        relay(away, late)
    for k in range(len(CHUNKS)):
        for chip in range(last + 1):
            source = 2 * chip + 1 - core
            copy(out.at[source], source, k, partner, 0).wait_recv()
    for when, origin, source, k, target, sem in sent:

        @pl.when(when)
        def _(origin=origin, source=source, k=k, target=target, sem=sem):
            copy(origin, source, k, target, sem).wait_send()

    here.wait()


def on_device(
    protein_pos, protein_vel, inv_mass, bond_atoms, left_atoms, right_atoms, water_pos, water_vel
):
    vmem = pl.BlockSpec(memory_space=pltpu.VMEM)
    hbm = pl.BlockSpec(memory_space=pltpu.HBM)
    count = lax.axis_size("dom")
    data, local, water_velocity = pl.pallas_call(
        share,
        out_shape=(
            jax.ShapeDtypeStruct((count, ROWS, 128), f32),
            jax.ShapeDtypeStruct((32, 128), f32),
            jax.ShapeDtypeStruct(water_pos.shape, f32),
        ),
        in_specs=[hbm] * 8,
        out_specs=(vmem,) * 3,
        scratch_shapes=[
            pltpu.VMEM(protein_pos.shape, f32),
            pltpu.VMEM(protein_vel.shape, f32),
            pltpu.VMEM((16, 128), f32),
            pltpu.VMEM(bond_atoms.shape, i32),
            pltpu.VMEM((3, 128), i32),
            pltpu.VMEM((3, 128), i32),
            pltpu.VMEM(water_pos.shape, f32),
            pltpu.VMEM(water_vel.shape, f32),
            pltpu.VMEM((ROWS, 128), f32),
            pltpu.VMEM((7, 16, 128), f32),
            pltpu.VMEM((32, 128), i32),
            pltpu.VMEM((24, 128), i32),
            pltpu.VMEM((24, 128), i32),
            pltpu.VMEM((32, 128), i32),
            pltpu.VMEM((8, 128), i32),
            pltpu.VMEM((18, 8, 128), f32),
            pltpu.SemaphoreType.DMA((17, len(CHUNKS))),
            pltpu.SemaphoreType.DMA((count, len(CHUNKS))),
            pltpu.SemaphoreType.DMA,
            pltpu.SemaphoreType.DMA((8,)),
        ],
        compiler_params=pltpu.CompilerParams(
            collective_id=0, has_side_effects=True, vmem_limit_bytes=16 * 2**20
        ),
        name="share",
    )(
        *(
            pltpu.with_memory_space_constraint(value, pltpu.HBM)
            for value in (
                protein_pos,
                protein_vel,
                inv_mass.reshape(16, 128),
                bond_atoms,
                left_atoms.reshape(3, 128),
                right_atoms.reshape(3, 128),
                water_pos,
                water_vel,
            )
        )
    )
    scratch = [
        ((3, E), f32), ((E,), f32), ((E,), f32),
        ((E,), i32), ((E,), i32), ((E,), i32), ((E,), i32),
        ((E,), f32), ((E,), f32), ((E,), f32),
        ((E,), f32), ((E,), f32),
        ((3, E), f32), ((3, E), f32), ((E,), f32), ((E,), f32), ((3, E), f32),
        ((3, S), f32), ((S,), f32), ((S,), i32), ((S,), i32), ((S,), f32),
        ((S,), f32), ((S,), f32), ((3, S), f32), ((S,), f32), ((S,), f32), ((3, S), f32),
        ((3, E), f32), ((E,), f32), ((3, S), f32),
    ]
    protein_velocity, water_velocity = pl.pallas_call(
        rounds,
        out_shape=(
            jax.ShapeDtypeStruct(protein_vel.shape, f32),
            jax.ShapeDtypeStruct(water_vel.shape, f32),
        ),
        in_specs=[vmem, vmem, hbm, vmem],
        out_specs=(vmem, hbm),
        scratch_shapes=[pltpu.VMEM(shape + (8, 128), kind) for shape, kind in scratch]
        + [pltpu.VMEM(protein_vel.shape, f32), pltpu.SemaphoreType.DMA, pltpu.SemaphoreType.DMA],
        compiler_params=pltpu.CompilerParams(vmem_limit_bytes=16 * 2**20),
        name="rounds",
    )(data, local, pltpu.with_memory_space_constraint(protein_vel, pltpu.HBM), water_velocity)
    return (protein_velocity, water_velocity)


def solution(mesh):
    in_specs = (
        P(None, ("rep", "dom")),
        P(None, ("rep", "dom")),
        P(("rep", "dom")),
        P(None, ("rep", "dom")),
        P(("rep", "dom")),
        P(("rep", "dom")),
        P(None, ("rep", "dom")),
        P(None, ("rep", "dom")),
    )
    out_specs = (P(None, ("rep", "dom")), P(None, ("rep", "dom")))
    return jax.shard_map(
        on_device, mesh=mesh, in_specs=in_specs, out_specs=out_specs, check_vma=False
    )
```
